128 devices in a mesh: blk: 32 (over y, x_hi, z), hid: 4 (over x_lo, core).
Axes of the slice: x: 4 (x_hi: 2, x_lo: 2; x = x_hi * 2 + x_lo), y: 4, z: 4, core: 2. Of those that a mesh axis runs over, the one named last changes fastest.
Arguments:
- queries: bfloat16 [3072, 128], P('blk'), may hold values from -6 to 6
- node_table: bfloat16 [65536, 128], P('blk'), may hold values from -6 to 6
- beam: int32 [3072, 128], P('blk'), may hold values from 0 to 65535, as said below
- w_query: bfloat16 [128, 256], P(None, 'hid'), may hold values from -0.5 to 0.5
- w_node: bfloat16 [128, 256], P(None, 'hid'), may hold values from -0.5 to 0.5
- w_cross: bfloat16 [128, 256], P(None, 'hid'), may hold values from -0.5 to 0.5
- bias_hidden: bfloat16 [256], P('hid'), may hold values from -3 to 3
- w_out: bfloat16 [256], P('hid'), may hold values from -0.375 to 0.375
Outputs:
- scores: float32 [3072, 128], P('blk', 'hid')
The draws below stay inside these ranges and needn't reach their ends.
Inputs may be any that keep to these rules, and one draw needn't show every extreme that they name: `beam`: each query's entries are distinct and come in sibling pairs 2p, 2p + 1 of 64 parents. Among the rows of one blk index (96 queries) at most 768 entries lie in any one aligned range of 2048 nodes, and some range holds exactly 768.
All inputs are finite; a program needn't handle non-finite values.
Results may differ from the reference program's by a relative error of at most 0.007.
Values may be sent and summed in bfloat16 or wider, within the bound.
A program may use at most 64 MiB of HBM per device.

```python
import math
import jax
import jax.numpy as jnp
from jax import lax

D = 128
HID = 256
BEAM = 128
NODES = 65536
Q_DEV = 96
QUERIES = 3072


def draw_beam(key, part):
    groups = QUERIES // Q_DEV
    parent_count = NODES // groups // 2
    per_owner = BEAM // 2 // groups
    most_slots = BEAM // groups
    stride = parent_count // most_slots
    key_hot, key_cold, key_start, key_order = jax.random.split(jax.random.fold_in(key, 17), 4)
    hottest = jax.random.randint(key_hot, (groups,), 0, groups)
    coldest = (hottest + 1 + jax.random.randint(key_cold, (groups,), 0, groups - 1)) % groups
    slots = jnp.arange(BEAM // 2, dtype=jnp.int32)
    base_owner = slots % groups
    base_index = slots // groups
    block_ids = jnp.arange(QUERIES, dtype=jnp.int32) // Q_DEV
    hot_rows = hottest[block_ids][:, None]
    cold_rows = coldest[block_ids][:, None]
    stolen = base_owner[None, :] == cold_rows
    owners = jnp.where(stolen, hot_rows, base_owner[None, :])
    within = jnp.where(stolen, base_index[None, :] + per_owner, base_index[None, :])
    starts = jax.random.randint(key_start, (QUERIES, groups), 0, parent_count)
    chosen = jnp.take_along_axis(starts, owners, axis=1)
    local_parent = (chosen + within * stride) % parent_count
    parents = owners * parent_count + local_parent
    children = jnp.stack([2 * parents, 2 * parents + 1], axis=-1).reshape(QUERIES, BEAM)
    row_keys = jax.random.split(key_order, QUERIES)
    orders = jax.vmap(lambda row_key: jax.random.permutation(row_key, BEAM))(row_keys)
    return jnp.take_along_axis(children, orders, axis=1).astype(jnp.int32)


def block_scale(key, extent, shards, smallest, largest):
    gain, own = 1.0, jax.random.fold_in(key, 6)
    for dim, blocks in shards:
        heights = jnp.exp(jax.random.uniform(jax.random.fold_in(own, dim), (blocks,), jnp.float32, smallest / len(shards), largest / len(shards)))
        gain = gain * jnp.repeat(heights, extent[dim] // blocks).reshape([-1 if axis == dim else 1 for axis in range(len(extent))])
    return gain


def gaussian(key, dims, deviation, reach, cuts=(), held_as=jnp.bfloat16):
    drawn = jax.random.normal(key, dims, jnp.float32) * deviation
    if len(cuts) > 0:
        drawn = block_scale(key, dims, cuts, -0.22, 0.18) * drawn
    return jnp.clip(drawn, min=-reach, max=reach).astype(held_as)


def setup_inputs(seed: int = 0) -> dict:
    streams_of = jax.random.split(jax.random.key(seed), 9)
    queries = gaussian(streams_of[0], (QUERIES, D), 1.0, 6.0, ((0, 32),))
    node_table = gaussian(streams_of[1], (NODES, D), 1.0, 6.0, ((0, 32),))
    beam = draw_beam(jax.random.fold_in(streams_of[8], 71), 0)
    w_query = gaussian(streams_of[3], (D, HID), D ** -0.5, 0.5, ((1, 4),))
    w_node = gaussian(streams_of[4], (D, HID), D ** -0.5, 0.5, ((1, 4),))
    w_cross = gaussian(streams_of[5], (D, HID), D ** -0.5, 0.5, ((1, 4),))
    bias_hidden = gaussian(streams_of[6], (HID,), 0.5, 3.0, ((0, 4),))
    w_out = gaussian(streams_of[7], (HID,), HID ** -0.5, 0.375, ((0, 4),))
    return {"queries": queries, "node_table": node_table, "beam": beam, "w_query": w_query, "w_node": w_node, "w_cross": w_cross, "bias_hidden": bias_hidden, "w_out": w_out}


def reference(queries, node_table, beam, w_query, w_node, w_cross, bias_hidden, w_out):
    block_size = math.gcd(QUERIES, 64)
    query_blocks = queries.reshape(QUERIES // block_size, block_size, D)
    beam_blocks = beam.reshape(QUERIES // block_size, block_size, BEAM)

    def score_block(operands):
        query_rows, beam_rows = operands
        picked = jnp.take(node_table, beam_rows, axis=0)
        cross = (query_rows[:, None, :].astype(jnp.float32) * picked.astype(jnp.float32)).astype(jnp.bfloat16)
        query_part = jnp.dot(query_rows, w_query, preferred_element_type=jnp.float32)
        node_part = jnp.dot(picked.reshape(-1, D), w_node, preferred_element_type=jnp.float32)
        node_part = node_part + jnp.dot(cross.reshape(-1, D), w_cross, preferred_element_type=jnp.float32)
        hidden = node_part.reshape(block_size, BEAM, HID) + query_part[:, None, :] + bias_hidden.astype(jnp.float32)
        hidden = jnp.maximum(hidden, 0.0)
        result = jnp.dot(hidden.reshape(-1, HID), w_out.astype(jnp.float32), precision=lax.Precision.HIGHEST)
        return result.reshape(block_size, BEAM)

    scores = lax.map(score_block, (query_blocks, beam_blocks))
    return scores.reshape(QUERIES, BEAM)
```

```python
import functools

import jax
import jax.numpy as jnp
from jax import lax
from jax.experimental import pallas as pl
from jax.experimental.pallas import tpu as pltpu
from jax.sharding import PartitionSpec as P

BF16, F32, I32 = jnp.bfloat16, jnp.float32, jnp.int32
GROUPS = 32
SHARES = 4
SERVED = GROUPS // SHARES
Q = 96
BEAM = 128
D = 128
HID = 256
HID_DEV = HID // SHARES
PARENTS = 1024
ROWS = 3
SLOTS = ROWS * 128
COLS = BEAM // SHARES
Q4 = Q // 4
MESH = pl.DeviceIdType.MESH


def nt(a, b):
    return lax.dot_general(a, b, (((1,), (1,)), ((), ())), preferred_element_type=F32)


def nn(a, b):
    return jnp.dot(a, b, preferred_element_type=F32)


def iota(shape, dim):
    return lax.broadcasted_iota(I32, shape, dim)


def flag(cond):
    return jnp.where(cond, 1.0, 0.0).astype(BF16)


def eye(n):
    return flag(iota((n, n), 0) == iota((n, n), 1))


def base_counts(group, even):
    lower = flag(iota((Q, Q), 0) > iota((Q, Q), 1))
    ones = jnp.ones((BEAM, BEAM), BF16)
    masks = [flag((group == i) & even) for i in range(SERVED)]
    before = nn(lower, jnp.concatenate(masks, axis=1)).astype(BF16)
    tall = jnp.concatenate([before[:, i * BEAM : (i + 1) * BEAM] for i in range(SERVED)], axis=0)
    total = nn(tall, ones)
    picked = jnp.zeros((Q, BEAM), F32)
    for i in range(SERVED):
        picked = jnp.where(group == i, total[i * Q : (i + 1) * Q], picked)
    return picked.astype(I32)


def kernel(
    q_ref, table_ref, beam_ref, wq_ref, wn_ref, wc_ref, vec_ref, out_ref,
    w_all, qbuf, req, reqbuf, ret, retbuf, tt, t32, inner, code_s, jl_s, a_s, b_s, wo_s, bi_s, code4, jl4, out4,
    q_send, q_recv, r_send, r_recv, w_send, w_recv, s_send, s_recv,
):
    b, h = lax.axis_index("blk"), lax.axis_index("hid")
    y, xh, z = b // 8, (b // 4) % 2, b % 4
    xl, core = h // 2, h % 2
    my_server = (y % 2) * 2 + z % 2
    my_place = (y // 2) * 4 + xh * 2 + z // 2
    own_xh = (xh + xl + y) % 2
    own_zl = 1 - core

    def owner_of(i):
        return (i // 2) * 8 + own_xh * 4 + (i % 2) * 2 + own_zl

    def source_of(k):
        return ((k // 4) * 2 + xl) * 8 + ((k // 2) % 2) * 4 + (k % 2) * 2 + core

    barrier = pltpu.get_barrier_semaphore()
    served_self = my_server == h

    @pl.loop(0, GROUPS)
    def _(o):
        @pl.when(jnp.logical_not(served_self & (o == b)))
        def _():
            pl.semaphore_signal(barrier, inc=1, device_id={"blk": o, "hid": my_server}, device_id_type=MESH)

    @pl.loop(0, SERVED)
    def _(k):
        for d in range(SHARES):
            @pl.when(jnp.logical_not((d == h) & (source_of(k) == b)))
            def _():
                pl.semaphore_signal(barrier, inc=1, device_id={"blk": source_of(k), "hid": d}, device_id_type=MESH)

    for d in range(1, SHARES):
        pl.semaphore_signal(barrier, inc=1, device_id={"blk": b, "hid": (h + d) % SHARES}, device_id_type=MESH)

    ident = eye(HID_DEV)
    vectors = jnp.concatenate(
        [jnp.broadcast_to(vec_ref[0:1, :], (64, HID_DEV)), jnp.broadcast_to(vec_ref[1:2, :], (64, HID_DEV))], axis=0
    ).astype(BF16)
    mine = jnp.concatenate(
        [nt(ident, wn_ref[...]), nt(ident, wc_ref[...]), nt(ident, wq_ref[...]), nt(ident, vectors)], axis=1
    ).astype(BF16)
    my_rows = pl.ds(pl.multiple_of(h * HID_DEV, HID_DEV), HID_DEV)
    w_all[my_rows, :] = mine

    beam = beam_ref[...]
    even = (beam & 1) == 0
    parent = beam >> 1
    owner = beam >> 11
    local = parent & (PARENTS - 1)
    keys = jnp.where(even, parent, 1 << 20)

    def count(t, acc):
        gap = parent - pltpu.roll(keys, t, 1)
        return acc + jnp.where((gap > 0) & (gap <= local), 1, 0)

    within = lax.fori_loop(1, BEAM, count, jnp.zeros((Q, BEAM), I32), unroll=False)
    inner[...] = within

    asked = ((owner >> 2) & 1 == own_xh) & ((owner & 1) == own_zl)
    group = jnp.where(asked, (owner >> 3) * 2 + ((owner >> 1) & 1), 64)
    rank = within + base_counts(group, even)
    code_s[...] = jnp.where(even, group * 4 + (rank >> 7), 999)
    jl_s[...] = rank & 127
    a_s[...] = (local & 255).astype(F32)
    b_s[...] = (iota((Q, BEAM), 0) + 96 * (local >> 8) - 192).astype(F32)

    pl.semaphore_wait(barrier, 2 * GROUPS + SHARES - 1 - jnp.where(served_self, 2, 0))

    def q_copy(i):
        return pltpu.make_async_remote_copy(
            src_ref=q_ref, dst_ref=qbuf.at[my_place], send_sem=q_send.at[i], recv_sem=q_recv.at[my_place],
            device_id={"blk": owner_of(i), "hid": my_server}, device_id_type=MESH,
        )

    def r_copy(i):
        return pltpu.make_async_remote_copy(
            src_ref=req.at[i], dst_ref=reqbuf.at[my_place], send_sem=r_send.at[i], recv_sem=r_recv.at[my_place],
            device_id={"blk": owner_of(i), "hid": my_server}, device_id_type=MESH,
        )

    def w_copy(d):
        return pltpu.make_async_remote_copy(
            src_ref=w_all.at[my_rows], dst_ref=w_all.at[my_rows], send_sem=w_send.at[d - 1], recv_sem=w_recv.at[d - 1],
            device_id={"blk": b, "hid": (h + d) % SHARES}, device_id_type=MESH,
        )

    @pl.loop(0, SERVED)
    def _(i):
        q_copy(i).start()

    row64 = iota((64, BEAM), 0)
    target = (row64 >> 3) * 4 + (row64 & 3)
    first_part = (row64 & 4) == 0
    lane_id = iota((BEAM, BEAM), 0)

    def compact(step, acc):
        values, places = [], []
        for u in range(2):
            at = pl.ds(2 * step + u, 1)
            payload = jnp.where(first_part, a_s[at, :], b_s[at, :])
            values.append(jnp.where(code_s[at, :] == target, payload, 0.0))
            places.append(jnp.where(lane_id == jl_s[at, :], 1.0, 0.0))
        return acc + nt(jnp.concatenate(values, axis=1).astype(BF16), jnp.concatenate(places, axis=1).astype(BF16))

    tables = lax.fori_loop(0, Q // 2, compact, jnp.zeros((64, BEAM), F32), unroll=False)
    for i in range(SERVED):
        req[i] = tables[8 * i : 8 * i + 8]

    @pl.loop(0, SERVED)
    def _(i):
        r_copy(i).start()

    for d in range(1, SHARES):
        w_copy(d).start()

    t32[...] = table_ref[...].astype(F32)
    ident = eye(D)
    for child in range(2):
        half = t32[pl.ds(child, PARENTS, stride=2), :].astype(BF16)
        tt[child * D : (child + 1) * D, :] = nt(ident, half).astype(BF16)

    def all_owners(g, acc):
        return acc + base_counts(owner - g * SERVED, even)

    rank = lax.fori_loop(0, GROUPS // SERVED, all_owners, inner[...], unroll=False)
    code = owner * 8 + (beam & 1) * 4 + (rank >> 7)
    lane, column = iota((BEAM, 4 * BEAM), 0), iota((BEAM, 4 * BEAM), 1)
    fold, column = column >> 7, column & 127
    select = flag(((column >> 5) == fold) & (lane == h * COLS + (column & 31)))
    for values, place in ((code, code4), (rank & 127, jl4)):
        wide = nn(values.astype(F32).astype(BF16), select)
        folded = jnp.zeros((Q4, BEAM), F32)
        for f in range(4):
            folded = folded + wide[f * Q4 : (f + 1) * Q4, f * BEAM : (f + 1) * BEAM]
        place[...] = folded.astype(I32)

    for d in range(1, SHARES):
        w_copy(d).wait_recv()
    bi_s[...] = jnp.broadcast_to(w_all[:, 3 * D : 3 * D + 1].astype(F32), (HID, 128))
    wo_s[...] = jnp.broadcast_to(w_all[:, 3 * D + 64 : 3 * D + 65].astype(F32), (HID, 128))

    def s_copy(k, d):
        return pltpu.make_async_remote_copy(
            src_ref=ret.at[k], dst_ref=retbuf.at[b], send_sem=s_send.at[k * SHARES + d], recv_sem=s_recv.at[b],
            device_id={"blk": source_of(k), "hid": d}, device_id_type=MESH,
        )

    @pl.loop(0, SERVED)
    def _(k):
        pltpu.make_async_remote_copy(
            src_ref=q_ref, dst_ref=qbuf.at[k], send_sem=q_send.at[k], recv_sem=q_recv.at[k],
            device_id={"blk": source_of(k), "hid": (h + 1) % SHARES}, device_id_type=MESH,
        ).wait_recv()
        pltpu.make_async_remote_copy(
            src_ref=req.at[k], dst_ref=reqbuf.at[k], send_sem=r_send.at[k], recv_sem=r_recv.at[k],
            device_id={"blk": source_of(k), "hid": (h + 1) % SHARES}, device_id_type=MESH,
        ).wait_recv()
        digits = reqbuf[k]
        low, rest = digits[0:4], digits[4:8] + 192.0
        high = jnp.where(rest >= 96.0, 1.0, 0.0) + jnp.where(rest >= 192.0, 1.0, 0.0) + jnp.where(rest >= 288.0, 1.0, 0.0)
        asking = (rest - 96.0 * high).astype(I32)
        wanted = (low + 256.0 * high).astype(I32)
        asking = jnp.concatenate([asking[r : r + 1] for r in range(ROWS)], axis=1)
        wanted = jnp.concatenate([wanted[r : r + 1] for r in range(ROWS)], axis=1)
        found = jnp.zeros((2 * D, SLOTS), F32)
        for c in range(PARENTS // 256):
            hot = flag(iota((256, SLOTS), 0) == wanted - 256 * c)
            found = found + nn(tt[:, c * 256 : (c + 1) * 256], hot)
        hot = flag(iota((Q, SLOTS), 0) == asking)
        query = nn(nt(eye(D), qbuf[k]).astype(BF16), hot)
        bias = jnp.concatenate([bi_s[...]] * ROWS, axis=1)
        weight = jnp.concatenate([wo_s[...]] * ROWS, axis=1)
        shared = nn(w_all[:, 2 * D : 3 * D], query.astype(BF16)) + bias
        rows = []
        for child in range(2):
            node = found[child * D : (child + 1) * D]
            joined = jnp.concatenate([node.astype(BF16), (node * query).astype(BF16)], axis=0)
            hidden = jnp.maximum(nn(w_all[:, : 2 * D], joined) + shared, 0.0)
            score = jnp.sum(hidden * weight, axis=0, keepdims=True)
            rows += [score[:, r * 128 : (r + 1) * 128] for r in range(ROWS)] + [jnp.zeros((1, 128), F32)]
        scores = jnp.concatenate(rows, axis=0)
        ret[k] = scores
        for d in range(SHARES):
            here = (d == h) & (source_of(k) == b)

            @pl.when(here)
            def _():
                retbuf[b] = scores

            @pl.when(jnp.logical_not(here))
            def _():
                s_copy(k, d).start()

    @pl.loop(0, GROUPS)
    def _(o):
        @pl.when(jnp.logical_not(served_self & (o == b)))
        def _():
            pltpu.make_async_remote_copy(
                src_ref=ret.at[0], dst_ref=retbuf.at[o], send_sem=s_send.at[0], recv_sem=s_recv.at[o],
                device_id={"blk": b, "hid": (h + 1) % SHARES}, device_id_type=MESH,
            ).wait_recv()

    table = retbuf[...].reshape(GROUPS * 8, 128)
    coarse = table.astype(BF16)
    fine = (table - coarse.astype(F32)).astype(BF16)
    slot_row = iota((GROUPS * 8, 2 * 128), 0)

    def read(step, carry):
        r0, r1 = pl.ds(2 * step, 1), pl.ds(2 * step + 1, 1)
        place = jnp.concatenate([jl4[r0, :], jl4[r1, :]], axis=1)
        which = jnp.concatenate([code4[r0, :], code4[r1, :]], axis=1)
        hot = flag(iota((128, 2 * 128), 0) == place)
        seen = nn(coarse, hot) + nn(fine, hot)
        score = jnp.sum(jnp.where(slot_row == which, seen, 0.0), axis=0, keepdims=True)
        out4[r0, :] = score[:, :128]
        out4[r1, :] = score[:, 128:]
        return carry

    lax.fori_loop(0, Q4 // 2, read, 0, unroll=False)
    for f in range(4):
        out_ref[f * Q4 : (f + 1) * Q4, :] = out4[:, f * COLS : (f + 1) * COLS]

    @pl.loop(0, SERVED)
    def _(i):
        q_copy(i).wait_send()
        r_copy(i).wait_send()
        for d in range(SHARES):
            @pl.when(jnp.logical_not((d == h) & (source_of(i) == b)))
            def _():
                s_copy(i, d).wait_send()

    for d in range(1, SHARES):
        w_copy(d).wait_send()


def shards(queries, node_table, beam, w_query, w_node, w_cross, bias_hidden, w_out):
    vectors = jnp.stack([bias_hidden, w_out]).astype(F32)
    dma = pltpu.SemaphoreType.DMA
    return pl.pallas_call(
        kernel,
        out_shape=jax.ShapeDtypeStruct((Q, COLS), F32),
        in_specs=[pl.BlockSpec(memory_space=pltpu.VMEM)] * 7,
        out_specs=pl.BlockSpec(memory_space=pltpu.VMEM),
        scratch_shapes=[
            pltpu.VMEM((HID, 4 * D), BF16),
            pltpu.VMEM((SERVED, Q, D), BF16),
            pltpu.VMEM((SERVED, 8, 128), F32),
            pltpu.VMEM((SERVED, 8, 128), F32),
            pltpu.VMEM((SERVED, 8, 128), F32),
            pltpu.VMEM((GROUPS, 8, 128), F32),
            pltpu.VMEM((2 * D, PARENTS), BF16),
            pltpu.VMEM((2 * PARENTS, D), F32),
            pltpu.VMEM((Q, BEAM), I32),
            pltpu.VMEM((Q, BEAM), I32),
            pltpu.VMEM((Q, BEAM), I32),
            pltpu.VMEM((Q, BEAM), F32),
            pltpu.VMEM((Q, BEAM), F32),
            pltpu.VMEM((HID, 128), F32),
            pltpu.VMEM((HID, 128), F32),
            pltpu.VMEM((Q4, 128), I32),
            pltpu.VMEM((Q4, 128), I32),
            pltpu.VMEM((Q4, 128), F32),
            dma((SERVED,)), dma((SERVED,)), dma((SERVED,)), dma((SERVED,)),
            dma((SHARES - 1,)), dma((SHARES - 1,)), dma((SERVED * SHARES,)), dma((GROUPS,)),
        ],
        compiler_params=pltpu.CompilerParams(collective_id=0, has_side_effects=True),
        name="beam_scores",
    )(queries, node_table, beam, w_query, w_node, w_cross, vectors)


def solution(mesh):
    in_specs = (
        P("blk", None),
        P("blk", None),
        P("blk", None),
        P(None, "hid"),
        P(None, "hid"),
        P(None, "hid"),
        P("hid"),
        P("hid"),
    )
    return jax.shard_map(shards, mesh=mesh, in_specs=in_specs, out_specs=P("blk", "hid"), check_vma=False)
```

```python
import functools

import jax
import jax.numpy as jnp
from jax import lax
from jax.experimental import pallas as pl
from jax.experimental.pallas import tpu as pltpu
from jax.sharding import PartitionSpec as P

BF16, F32, I32 = jnp.bfloat16, jnp.float32, jnp.int32
GROUPS = 32
SHARES = 4
SERVED = GROUPS // SHARES
Q = 96
BEAM = 128
D = 128
HID = 256
HID_DEV = HID // SHARES
PARENTS = 1024
ROWS = 3
SLOTS = ROWS * 128
COLS = BEAM // SHARES
PAIR = 2
MESH = pl.DeviceIdType.MESH


def nt(a, b):
    return lax.dot_general(a, b, (((1,), (1,)), ((), ())), preferred_element_type=F32)


def nn(a, b):
    return jnp.dot(a, b, preferred_element_type=F32)


def iota(shape, dim):
    return lax.broadcasted_iota(I32, shape, dim)


def flag(cond):
    return jnp.where(cond, 1.0, 0.0).astype(BF16)


def eye(n):
    return flag(iota((n, n), 0) == iota((n, n), 1))


def wide_row(row, copies):
    return jnp.concatenate([jnp.broadcast_to(row, (16, row.shape[1])).astype(BF16)] * copies, axis=0)


def one_hot(row, height):
    row = wide_row(row, height // 16)
    return jnp.where(iota((height, row.shape[1]), 0).astype(F32).astype(BF16) == row, 1.0, 0.0).astype(BF16)


def list_starts(owner, even, ids):
    lower = flag(iota((Q, Q), 0) > iota((Q, Q), 1))
    ones = jnp.ones((BEAM, BEAM), BF16)
    masks = [flag((owner == o) & even) for o in ids]
    before = nn(lower, jnp.concatenate(masks, axis=1))
    tall = [
        before[:, i * BEAM : (i + 1) * BEAM] - jnp.where((owner < o) & even, 1.0, 0.0) for i, o in enumerate(ids)
    ]
    total = nn(jnp.concatenate(tall, axis=0).astype(BF16), ones)
    picked = jnp.zeros((Q, BEAM), F32)
    for i, o in enumerate(ids):
        picked = jnp.where(owner == o, total[i * Q : (i + 1) * Q], picked)
    return picked.astype(I32)


def kernel(
    q_hbm, table_hbm, beam_hbm, wq_hbm, wn_hbm, wc_hbm, bias_hbm, wout_hbm, out_ref,
    q_ref, table_ref, beam_ref, w_in, bias_in, wout_in,
    w_all, qbuf, req, reqbuf, ret, retbuf, tt, t32, inner, code_s, jl_s, a_s, b_s, wo_s, bi_s,
    in_sem, q_send, q_recv, r_send, r_recv, w_send, w_recv, s_send, s_recv,
):
    b, h = lax.axis_index("blk"), lax.axis_index("hid")
    y, xh, z = b // 8, (b // 4) % 2, b % 4
    xl, core = h // 2, h % 2
    my_server = (y % 2) * 2 + z % 2
    my_place = (y // 2) * 4 + xh * 2 + z // 2
    own_xh = (xh + xl + y) % 2
    own_zl = 1 - core

    def owner_of(i):
        return (i // 2) * 8 + own_xh * 4 + (i % 2) * 2 + own_zl

    def source_of(k):
        return ((k // 4) * 2 + xl) * 8 + ((k // 2) % 2) * 4 + (k % 2) * 2 + core

    loads = [
        pltpu.make_async_copy(src, dst, in_sem.at[n])
        for n, (src, dst) in enumerate((
            (beam_hbm, beam_ref), (wn_hbm, w_in.at[0]), (wc_hbm, w_in.at[1]), (wq_hbm, w_in.at[2]),
            (bias_hbm, bias_in), (wout_hbm, wout_in), (q_hbm, q_ref), (table_hbm, table_ref),
        ))
    ]
    for load in loads:
        load.start()

    barrier = pltpu.get_barrier_semaphore()
    served_self = my_server == h

    @pl.loop(0, GROUPS)
    def _(o):
        @pl.when(jnp.logical_not(served_self & (o == b)))
        def _():
            pl.semaphore_signal(barrier, inc=1, device_id={"blk": o, "hid": my_server}, device_id_type=MESH)

    @pl.loop(0, SERVED)
    def _(k):
        sender = lax.rem(xl + xh + (k // 2) % 2, 2) * 2 + 1 - z % 2
        pl.semaphore_signal(barrier, inc=1, device_id={"blk": source_of(k), "hid": sender}, device_id_type=MESH)

    for d in range(1, SHARES):
        pl.semaphore_signal(barrier, inc=1, device_id={"blk": b, "hid": (h + d) % SHARES}, device_id_type=MESH)

    for load in loads[:7]:
        load.wait()

    beam = beam_ref[...]
    even = (beam & 1) == 0
    parent = beam >> 1
    owner = beam >> 11
    local = parent & (PARENTS - 1)
    keys = jnp.where(even, parent, 1 << 20)

    def count(step, acc):
        for u in range(8):
            acc = acc + jnp.where(pltpu.roll(keys, 8 * step + u, 1) < parent, 1, 0)
        return acc

    below = lax.fori_loop(0, BEAM // 8, count, jnp.zeros((Q, BEAM), I32), unroll=False)
    inner[...] = below

    asked = ((owner >> 2) & 1 == own_xh) & ((owner & 1) == own_zl)
    group = jnp.where(asked, (owner >> 3) * 2 + ((owner >> 1) & 1), 64)
    rank = below + list_starts(owner, even, [owner_of(i) for i in range(SERVED)])
    code_s[...] = jnp.where(even & asked, group * 4 + (rank >> 7), 64).astype(F32)
    jl_s[...] = (rank & 127).astype(F32)
    a_s[...] = (local & 255).astype(F32)
    b_s[...] = (iota((Q, BEAM), 0) + 96 * (local >> 8) - 192).astype(F32)

    row64 = iota((64, BEAM), 0)
    target = ((row64 >> 3) * 4 + (row64 & 3)).astype(F32).astype(BF16)
    is_b = ((iota((16, BEAM), 0) >> 2) & 1).astype(F32).astype(BF16)
    is_a = 1 - is_b

    def compact(step, acc):
        values, places = [], []
        for u in range(16):
            at = pl.ds(16 * step + u, 1)
            payload = is_a * wide_row(a_s[at, :], 1) + is_b * wide_row(b_s[at, :], 1)
            payload = jnp.concatenate([payload] * 4, axis=0)
            values.append(jnp.where(wide_row(code_s[at, :], 4) == target, payload, 0.0).astype(BF16))
            places.append(one_hot(jl_s[at, :], BEAM))
        return acc + nt(jnp.concatenate(values, axis=1), jnp.concatenate(places, axis=1))

    tables = lax.fori_loop(0, Q // 16, compact, jnp.zeros((64, BEAM), F32), unroll=False)
    for i in range(SERVED):
        req[i] = tables[8 * i : 8 * i + 8]

    ident = eye(HID_DEV)
    vectors = jnp.concatenate(
        [jnp.broadcast_to(v[...].astype(F32), (64, HID_DEV)) for v in (bias_in, wout_in)], axis=0
    ).astype(BF16)
    my_rows = pl.ds(pl.multiple_of(h * HID_DEV, HID_DEV), HID_DEV)
    for n in range(3):
        w_all[my_rows, n * D : (n + 1) * D] = w_in[n]
    w_all[my_rows, 3 * D :] = nt(ident, vectors).astype(BF16)

    pl.semaphore_wait(barrier, GROUPS + SERVED + SHARES - 1 - jnp.where(served_self, 1, 0))

    def q_copy(i):
        return pltpu.make_async_remote_copy(
            src_ref=q_ref, dst_ref=qbuf.at[my_place], send_sem=q_send.at[i], recv_sem=q_recv.at[my_place],
            device_id={"blk": owner_of(i), "hid": my_server}, device_id_type=MESH,
        )

    def r_copy(i):
        return pltpu.make_async_remote_copy(
            src_ref=req.at[i], dst_ref=reqbuf.at[my_place], send_sem=r_send.at[i], recv_sem=r_recv.at[my_place],
            device_id={"blk": owner_of(i), "hid": my_server}, device_id_type=MESH,
        )

    def w_copy(d):
        return pltpu.make_async_remote_copy(
            src_ref=w_all.at[my_rows], dst_ref=w_all.at[my_rows], send_sem=w_send.at[d - 1], recv_sem=w_recv.at[d - 1],
            device_id={"blk": b, "hid": (h + d) % SHARES}, device_id_type=MESH,
        )

    @pl.loop(0, SERVED)
    def _(i):
        q_copy(i).start()
        r_copy(i).start()

    for d in range(1, SHARES):
        w_copy(d).start()

    loads[7].wait()
    t32[...] = table_ref[...].astype(F32)
    ident = eye(D)
    for child in range(2):
        half = t32[pl.ds(child, PARENTS, stride=2), :].astype(BF16)
        tt[child * D : (child + 1) * D, :] = nt(ident, half).astype(BF16)

    def all_owners(g, acc):
        return acc + list_starts(owner, even, [g * SERVED + i for i in range(SERVED)])

    rank = lax.fori_loop(0, GROUPS // SERVED, all_owners, inner[...], unroll=False)
    code = owner * 8 + (beam & 1) * 4 + (rank >> 7)
    mine = flag(iota((COLS, BEAM), 1) == iota((COLS, BEAM), 0) + h * COLS)
    pad = jnp.zeros((BEAM - Q, BEAM), F32)

    def columns(values):
        return nt(mine, jnp.concatenate([values.astype(F32), pad], axis=0).astype(BF16))

    code_t, jl_t = columns(code), columns(rank & 127)

    for d in range(1, SHARES):
        w_copy(d).wait_recv()
    bi_s[...] = jnp.broadcast_to(w_all[:, 3 * D : 3 * D + 1].astype(F32), (HID, 128))
    wo_s[...] = jnp.broadcast_to(w_all[:, 3 * D + 64 : 3 * D + 65].astype(F32), (HID, 128))

    def s_copy(k, d):
        return pltpu.make_async_remote_copy(
            src_ref=ret.at[k], dst_ref=retbuf.at[b], send_sem=s_send.at[k * SHARES + d], recv_sem=s_recv.at[b],
            device_id={"blk": source_of(k), "hid": d}, device_id_type=MESH,
        )

    def score(k):
        digits = reqbuf[k]
        low, rest = digits[0:4], digits[4:8] + 192.0
        high = jnp.where(rest >= 96.0, 1.0, 0.0) + jnp.where(rest >= 192.0, 1.0, 0.0) + jnp.where(rest >= 288.0, 1.0, 0.0)
        asking = rest - 96.0 * high
        wanted = low + 256.0 * high
        asking = jnp.concatenate([asking[r : r + 1] for r in range(ROWS)], axis=1)
        wanted = jnp.concatenate([wanted[r : r + 1] for r in range(ROWS)], axis=1)
        hot = jnp.concatenate([one_hot(wanted - 256.0 * c, 256) for c in range(PARENTS // 256)], axis=0)
        found = nn(tt[...], hot)
        query = nn(nt(eye(D), qbuf[k]).astype(BF16), one_hot(asking, Q))
        bias = jnp.concatenate([bi_s[...]] * ROWS, axis=1)
        weight = jnp.concatenate([wo_s[...]] * ROWS, axis=1)
        shared = nn(w_all[:, 2 * D : 3 * D], query.astype(BF16)) + bias
        rows = []
        for child in range(2):
            node = found[child * D : (child + 1) * D]
            joined = jnp.concatenate([node.astype(BF16), (node * query).astype(BF16)], axis=0)
            hidden = jnp.maximum(nn(w_all[:, : 2 * D], joined) + shared, 0.0)
            total = jnp.sum(hidden * weight, axis=0, keepdims=True)
            rows += [total[:, r * 128 : (r + 1) * 128] for r in range(ROWS)] + [jnp.zeros((1, 128), F32)]
        return jnp.concatenate(rows, axis=0)

    @pl.loop(0, SERVED // PAIR)
    def _(pair):
        for u in range(PAIR):
            k = PAIR * pair + u
            pltpu.make_async_remote_copy(
                src_ref=q_ref, dst_ref=qbuf.at[k], send_sem=q_send.at[k], recv_sem=q_recv.at[k],
                device_id={"blk": source_of(k), "hid": (h + 1) % SHARES}, device_id_type=MESH,
            ).wait_recv()
            pltpu.make_async_remote_copy(
                src_ref=req.at[k], dst_ref=reqbuf.at[k], send_sem=r_send.at[k], recv_sem=r_recv.at[k],
                device_id={"blk": source_of(k), "hid": (h + 1) % SHARES}, device_id_type=MESH,
            ).wait_recv()
        for u in range(PAIR):
            ret[PAIR * pair + u] = score(PAIR * pair + u)
        for u in range(PAIR):
            k = PAIR * pair + u
            for d in range(SHARES):
                here = (d == h) & (source_of(k) == b)

                @pl.when(here)
                def _():
                    retbuf[b] = ret[k]

                @pl.when(jnp.logical_not(here))
                def _():
                    s_copy(k, d).start()

    @pl.loop(0, GROUPS)
    def _(o):
        @pl.when(jnp.logical_not(served_self & (o == b)))
        def _():
            pltpu.make_async_remote_copy(
                src_ref=ret.at[0], dst_ref=retbuf.at[o], send_sem=s_send.at[0], recv_sem=s_recv.at[o],
                device_id={"blk": b, "hid": (h + 1) % SHARES}, device_id_type=MESH,
            ).wait_recv()

    table = retbuf[...].reshape(GROUPS * 8, 128)
    coarse = table.astype(BF16)
    fine = (table - coarse.astype(F32)).astype(BF16)
    slot_row = iota((GROUPS * 8, 2 * 128), 0).astype(F32)
    for c in range(0, COLS, 2):
        hot = one_hot(jnp.concatenate([jl_t[c : c + 1], jl_t[c + 1 : c + 2]], axis=1), 128)
        which = jnp.concatenate([code_t[c : c + 1], code_t[c + 1 : c + 2]], axis=1)
        seen = nn(coarse, hot) + nn(fine, hot)
        total = jnp.sum(jnp.where(slot_row == which, seen, 0.0), axis=0, keepdims=True)
        out_ref[c : c + 1, :] = total[:, :Q]
        out_ref[c + 1 : c + 2, :] = total[:, 128 : 128 + Q]

    @pl.loop(0, SERVED)
    def _(i):
        q_copy(i).wait_send()
        r_copy(i).wait_send()
        for d in range(SHARES):
            @pl.when(jnp.logical_not((d == h) & (source_of(i) == b)))
            def _():
                s_copy(i, d).wait_send()

    for d in range(1, SHARES):
        w_copy(d).wait_send()


def shards(queries, node_table, beam, w_query, w_node, w_cross, bias_hidden, w_out):
    dma = pltpu.SemaphoreType.DMA
    scores = pl.pallas_call(
        kernel,
        out_shape=jax.ShapeDtypeStruct((COLS, Q), F32),
        in_specs=[pl.BlockSpec(memory_space=pl.ANY)] * 8,
        out_specs=pl.BlockSpec(memory_space=pltpu.VMEM),
        scratch_shapes=[
            pltpu.VMEM((Q, D), BF16),
            pltpu.VMEM((2 * PARENTS, D), BF16),
            pltpu.VMEM((Q, BEAM), I32),
            pltpu.VMEM((3, HID_DEV, D), BF16),
            pltpu.VMEM((1, HID_DEV), BF16),
            pltpu.VMEM((1, HID_DEV), BF16),
            pltpu.VMEM((HID, 4 * D), BF16),
            pltpu.VMEM((SERVED, Q, D), BF16),
            pltpu.VMEM((SERVED, 8, 128), F32),
            pltpu.VMEM((SERVED, 8, 128), F32),
            pltpu.VMEM((SERVED, 8, 128), F32),
            pltpu.VMEM((GROUPS, 8, 128), F32),
            pltpu.VMEM((2 * D, PARENTS), BF16),
            pltpu.VMEM((2 * PARENTS, D), F32),
            pltpu.VMEM((Q, BEAM), I32),
            pltpu.VMEM((Q, BEAM), F32),
            pltpu.VMEM((Q, BEAM), F32),
            pltpu.VMEM((Q, BEAM), F32),
            pltpu.VMEM((Q, BEAM), F32),
            pltpu.VMEM((HID, 128), F32),
            pltpu.VMEM((HID, 128), F32),
            dma((8,)), dma((SERVED,)), dma((SERVED,)), dma((SERVED,)), dma((SERVED,)),
            dma((SHARES - 1,)), dma((SHARES - 1,)), dma((SERVED * SHARES,)), dma((GROUPS,)),
        ],
        compiler_params=pltpu.CompilerParams(collective_id=0, has_side_effects=True),
        name="beam_scores",
    )(
        queries, node_table, beam, w_query.T, w_node.T, w_cross.T,
        bias_hidden.reshape(1, HID_DEV), w_out.reshape(1, HID_DEV),
    )
    return scores.T


def solution(mesh):
    in_specs = (
        P("blk", None),
        P("blk", None),
        P("blk", None),
        P(None, "hid"),
        P(None, "hid"),
        P(None, "hid"),
        P("hid"),
        P("hid"),
    )
    return jax.shard_map(shards, mesh=mesh, in_specs=in_specs, out_specs=P("blk", "hid"), check_vma=False)
```

```python
import functools

import jax
import jax.numpy as jnp
from jax import lax
from jax.experimental import pallas as pl
from jax.experimental.pallas import tpu as pltpu
from jax.sharding import PartitionSpec as P

BF16, F32, I32 = jnp.bfloat16, jnp.float32, jnp.int32
RANK = jnp.int16
GROUPS = 32
SHARES = 4
SERVED = GROUPS // SHARES
Q = 96
BEAM = 128
D = 128
HID = 256
HID_DEV = HID // SHARES
PARENTS = 1024
ROWS = 3
SLOTS = ROWS * 128
COLS = BEAM // SHARES
STEP = 32
PAIR = 2
MESH = pl.DeviceIdType.MESH


def nt(a, b):
    return lax.dot_general(a, b, (((1,), (1,)), ((), ())), preferred_element_type=F32)


def nn(a, b):
    return jnp.dot(a, b, preferred_element_type=F32)


def iota(shape, dim):
    return lax.broadcasted_iota(I32, shape, dim)


def flag(cond):
    return jnp.where(cond, 1.0, 0.0).astype(BF16)


def eye(n):
    return flag(iota((n, n), 0) == iota((n, n), 1))


def wide_row(row, copies):
    return jnp.concatenate([jnp.broadcast_to(row, (16, row.shape[1])).astype(BF16)] * copies, axis=0)


def one_hot(row, height):
    row = wide_row(row, height // 16)
    match = iota((height, row.shape[1]), 0).astype(F32).astype(BF16) == row
    return jnp.where(match, jnp.ones(row.shape, BF16), jnp.zeros(row.shape, BF16))


def list_starts(owner, even, ids):
    lower = flag(iota((Q, Q), 0) > iota((Q, Q), 1))
    ones = jnp.ones((BEAM, BEAM), BF16)
    masks = [flag((owner == o) & even) for o in ids]
    before = nn(lower, jnp.concatenate(masks, axis=1))
    tall = [
        before[:, i * BEAM : (i + 1) * BEAM] - jnp.where((owner < o) & even, 1.0, 0.0) for i, o in enumerate(ids)
    ]
    total = nn(jnp.concatenate(tall, axis=0).astype(BF16), ones)
    picked = jnp.zeros((Q, BEAM), F32)
    for i, o in enumerate(ids):
        picked = jnp.where(owner == o, total[i * Q : (i + 1) * Q], picked)
    return picked.astype(I32)


def kernel(
    q_hbm, table_hbm, beam_hbm, wq_hbm, wn_hbm, wc_hbm, bias_hbm, wout_hbm, out_ref,
    q_ref, table_ref, beam_ref, w_in, bias_in, wout_in,
    w_all, qbuf, req, reqbuf, ret, retbuf, tt, t32, keys, inner, code_s, jl_s, a_s, b_s, wo_s, bi_s,
    in_sem, q_send, q_recv, r_send, r_recv, w_send, w_recv, s_send, s_recv,
):
    b, h = lax.axis_index("blk"), lax.axis_index("hid")
    y, xh, z = b // 8, (b // 4) % 2, b % 4
    xl, core = h // 2, h % 2
    my_server = (y % 2) * 2 + z % 2
    my_place = (y // 2) * 4 + xh * 2 + z // 2
    own_xh = (xh + xl + y) % 2
    own_zl = 1 - core

    def owner_of(i):
        return (i // 2) * 8 + own_xh * 4 + (i % 2) * 2 + own_zl

    def source_of(k):
        return ((k // 4) * 2 + xl) * 8 + ((k // 2) % 2) * 4 + (k % 2) * 2 + core

    loads = [
        pltpu.make_async_copy(src, dst, in_sem.at[n])
        for n, (src, dst) in enumerate((
            (beam_hbm, beam_ref), (wn_hbm, w_in.at[0]), (wc_hbm, w_in.at[1]), (wq_hbm, w_in.at[2]),
            (bias_hbm, bias_in), (wout_hbm, wout_in), (q_hbm, q_ref), (table_hbm, table_ref),
        ))
    ]
    for load in loads:
        load.start()

    barrier = pltpu.get_barrier_semaphore()
    served_self = my_server == h

    for k in range(SERVED):
        sender = lax.rem(xl + xh + (k // 2) % 2, 2) * 2 + 1 - z % 2
        pl.semaphore_signal(barrier, inc=1, device_id={"blk": source_of(k), "hid": sender}, device_id_type=MESH)

    for d in range(1, SHARES):
        pl.semaphore_signal(barrier, inc=1, device_id={"blk": b, "hid": (h + d) % SHARES}, device_id_type=MESH)

    for load in loads[:7]:
        load.wait()

    beam = beam_ref[...]
    even = (beam & 1) == 0
    owner = beam >> 11
    local = (beam >> 1) & (PARENTS - 1)
    tall = jnp.concatenate([beam, jnp.zeros((BEAM - Q, BEAM), I32)], axis=0).T
    parent = (tall >> 1).astype(RANK)
    keys[...] = jnp.where((tall & 1) == 0, tall >> 1, 32767)

    def count(step, acc):
        for u in range(16):
            row = jnp.broadcast_to(keys[pl.ds(16 * step + u, 1), :], (16, 128)).astype(RANK)
            row = jnp.concatenate([row] * 8, axis=0)
            acc = acc + jnp.where(row < parent, jnp.ones(acc.shape, RANK), jnp.zeros(acc.shape, RANK))
        return acc

    below = lax.fori_loop(0, BEAM // 16, count, jnp.zeros((BEAM, BEAM), RANK), unroll=False)
    below = below.astype(I32).T[:Q]
    inner[...] = below

    asked = ((owner >> 2) & 1 == own_xh) & ((owner & 1) == own_zl)
    group = jnp.where(asked, (owner >> 3) * 2 + ((owner >> 1) & 1), 64)
    rank = below + list_starts(owner, even, [owner_of(i) for i in range(SERVED)])
    code_s[...] = jnp.where(even & asked, group * 4 + (rank >> 7), 64).astype(F32)
    jl_s[...] = (rank & 127).astype(F32)
    a_s[...] = (local & 255).astype(F32)
    b_s[...] = (iota((Q, BEAM), 0) + 96 * (local >> 8) - 192).astype(F32)

    row64 = iota((64, BEAM), 0)
    target = ((row64 >> 3) * 4 + (row64 & 3)).astype(F32).astype(BF16)
    is_b = ((iota((16, BEAM), 0) >> 2) & 1).astype(F32).astype(BF16)
    is_a = 1 - is_b

    def compact(step, acc):
        values, places = [], []
        for u in range(STEP):
            at = pl.ds(STEP * step + u, 1)
            payload = is_a * wide_row(a_s[at, :], 1) + is_b * wide_row(b_s[at, :], 1)
            payload = jnp.concatenate([payload] * 4, axis=0)
            values.append(jnp.where(wide_row(code_s[at, :], 4) == target, payload, 0.0).astype(BF16))
            places.append(one_hot(jl_s[at, :], BEAM))
        return acc + nt(jnp.concatenate(values, axis=1), jnp.concatenate(places, axis=1))

    tables = lax.fori_loop(0, Q // STEP, compact, jnp.zeros((64, BEAM), F32), unroll=False)
    for i in range(SERVED):
        req[i] = tables[8 * i : 8 * i + 8]

    ident = eye(HID_DEV)
    vectors = jnp.concatenate(
        [jnp.broadcast_to(v[...].astype(F32), (64, HID_DEV)) for v in (bias_in, wout_in)], axis=0
    ).astype(BF16)
    my_rows = pl.ds(pl.multiple_of(h * HID_DEV, HID_DEV), HID_DEV)
    for n in range(3):
        w_all[my_rows, n * D : (n + 1) * D] = w_in[n]
    w_all[my_rows, 3 * D :] = nt(ident, vectors).astype(BF16)

    pl.semaphore_wait(barrier, SERVED + SHARES - 1)

    def q_copy(i):
        return pltpu.make_async_remote_copy(
            src_ref=q_ref, dst_ref=qbuf.at[my_place], send_sem=q_send.at[i], recv_sem=q_recv.at[my_place],
            device_id={"blk": owner_of(i), "hid": my_server}, device_id_type=MESH,
        )

    def r_copy(i):
        return pltpu.make_async_remote_copy(
            src_ref=req.at[i], dst_ref=reqbuf.at[my_place], send_sem=r_send.at[i], recv_sem=r_recv.at[my_place],
            device_id={"blk": owner_of(i), "hid": my_server}, device_id_type=MESH,
        )

    def w_copy(d):
        return pltpu.make_async_remote_copy(
            src_ref=w_all.at[my_rows], dst_ref=w_all.at[my_rows], send_sem=w_send.at[d - 1], recv_sem=w_recv.at[d - 1],
            device_id={"blk": b, "hid": (h + d) % SHARES}, device_id_type=MESH,
        )

    for d in range(1, SHARES):
        w_copy(d).start()

    @pl.loop(0, SERVED)
    def _(n):
        i = lax.rem(y + 2 + n // 2, 4) * 2 + lax.rem(z // 2 + 1 + n, 2)
        q_copy(i).start()
        r_copy(i).start()

    loads[7].wait()
    t32[...] = table_ref[...].astype(F32)
    ident = eye(D)
    for child in range(2):
        half = t32[pl.ds(child, PARENTS, stride=2), :].astype(BF16)
        tt[child * D : (child + 1) * D, :] = nt(ident, half).astype(BF16)

    def all_owners(g, acc):
        return acc + list_starts(owner, even, [g * SERVED + i for i in range(SERVED)])

    rank = lax.fori_loop(0, GROUPS // SERVED, all_owners, inner[...], unroll=False)
    code = owner * 4 + (rank >> 7)
    mine = flag(iota((COLS, BEAM), 1) == iota((COLS, BEAM), 0) + h * COLS)
    pad = jnp.zeros((BEAM - Q, BEAM), F32)

    def columns(values):
        return nt(mine, jnp.concatenate([values.astype(F32), pad], axis=0).astype(BF16))

    code_t, jl_t = columns(code), columns((beam & 1) * 128 + (rank & 127))

    def s_copy(k, d):
        return pltpu.make_async_remote_copy(
            src_ref=ret.at[k], dst_ref=retbuf.at[b], send_sem=s_send.at[k * SHARES + d], recv_sem=s_recv.at[b],
            device_id={"blk": source_of(k), "hid": d}, device_id_type=MESH,
        )

    def gather(k):
        digits = reqbuf[k]
        low, rest = digits[0:4], digits[4:8] + 192.0
        high = jnp.where(rest >= 96.0, 1.0, 0.0) + jnp.where(rest >= 192.0, 1.0, 0.0) + jnp.where(rest >= 288.0, 1.0, 0.0)
        asking = rest - 96.0 * high
        wanted = low + 256.0 * high
        asking = jnp.concatenate([asking[r : r + 1] for r in range(ROWS)], axis=1)
        wanted = jnp.concatenate([wanted[r : r + 1] for r in range(ROWS)], axis=1)
        hot = jnp.concatenate([one_hot(wanted - 256.0 * c, 256) for c in range(PARENTS // 256)], axis=0)
        found = nn(tt[...], hot)
        query = nn(nt(eye(D), qbuf[k]).astype(BF16), one_hot(asking, Q))
        return found, query

    def score(found, query):
        bias = jnp.concatenate([bi_s[...]] * ROWS, axis=1)
        weight = jnp.concatenate([wo_s[...]] * ROWS, axis=1)
        shared = nn(w_all[:, 2 * D : 3 * D], query.astype(BF16)) + bias
        rows = []
        for child in range(2):
            node = found[child * D : (child + 1) * D]
            joined = jnp.concatenate([node.astype(BF16), (node * query).astype(BF16)], axis=0)
            hidden = jnp.maximum(nn(w_all[:, : 2 * D], joined) + shared, 0.0)
            total = jnp.sum(hidden * weight, axis=0, keepdims=True)
            rows += [total[:, r * 128 : (r + 1) * 128] for r in range(ROWS)] + [jnp.zeros((1, 128), F32)]
        return jnp.concatenate(rows, axis=0)

    def near(n):
        a = lax.rem(y // 2 + n // 4, 2)
        e = lax.rem(xh + n, 2)
        return a * 4 + e * 2 + lax.rem(z // 2 + n // 2, 2)

    @pl.loop(0, SERVED // PAIR)
    def _(pair):
        places = [near(PAIR * pair + u) for u in range(PAIR)]
        for k in places:
            pltpu.make_async_remote_copy(
                src_ref=q_ref, dst_ref=qbuf.at[k], send_sem=q_send.at[k], recv_sem=q_recv.at[k],
                device_id={"blk": source_of(k), "hid": (h + 1) % SHARES}, device_id_type=MESH,
            ).wait_recv()
            pltpu.make_async_remote_copy(
                src_ref=req.at[k], dst_ref=reqbuf.at[k], send_sem=r_send.at[k], recv_sem=r_recv.at[k],
                device_id={"blk": source_of(k), "hid": (h + 1) % SHARES}, device_id_type=MESH,
            ).wait_recv()
        gathered = [gather(k) for k in places]

        @pl.when(pair == 0)
        def _():
            for d in range(1, SHARES):
                w_copy(d).wait_recv()
            bi_s[...] = jnp.broadcast_to(w_all[:, 3 * D : 3 * D + 1].astype(F32), (HID, 128))
            wo_s[...] = jnp.broadcast_to(w_all[:, 3 * D + 64 : 3 * D + 65].astype(F32), (HID, 128))

        for k, (found, query) in zip(places, gathered):
            ret[k] = score(found, query)
        for k in places:
            for d in range(SHARES):
                here = (d == h) & (source_of(k) == b)

                @pl.when(here)
                def _():
                    retbuf[b] = ret[k]

                @pl.when(jnp.logical_not(here))
                def _():
                    s_copy(k, d).start()

    @pl.loop(0, GROUPS)
    def _(o):
        @pl.when(jnp.logical_not(served_self & (o == b)))
        def _():
            pltpu.make_async_remote_copy(
                src_ref=ret.at[0], dst_ref=retbuf.at[o], send_sem=s_send.at[0], recv_sem=s_recv.at[o],
                device_id={"blk": b, "hid": (h + 1) % SHARES}, device_id_type=MESH,
            ).wait_recv()

    table = jnp.concatenate(
        [retbuf[:, 4 * child : 4 * child + 4, :].reshape(GROUPS * 4, 128) for child in range(2)], axis=1
    )
    coarse = table.astype(BF16)
    parts = jnp.concatenate([coarse, (table - coarse.astype(F32)).astype(BF16)], axis=0)
    slot_row = iota((GROUPS * 4, 2 * 128), 0).astype(F32)
    for c in range(0, COLS, 2):
        hot = one_hot(jnp.concatenate([jl_t[c : c + 1], jl_t[c + 1 : c + 2]], axis=1), 256)
        which = jnp.concatenate([code_t[c : c + 1], code_t[c + 1 : c + 2]], axis=1)
        seen = nn(parts, hot)
        seen = seen[: GROUPS * 4] + seen[GROUPS * 4 :]
        total = jnp.sum(jnp.where(slot_row == which, seen, 0.0), axis=0, keepdims=True)
        out_ref[c : c + 1, :] = total[:, :Q]
        out_ref[c + 1 : c + 2, :] = total[:, 128 : 128 + Q]

    @pl.loop(0, SERVED)
    def _(i):
        q_copy(i).wait_send()
        r_copy(i).wait_send()
        for d in range(SHARES):
            @pl.when(jnp.logical_not((d == h) & (source_of(i) == b)))
            def _():
                s_copy(i, d).wait_send()

    for d in range(1, SHARES):
        w_copy(d).wait_send()


def shards(queries, node_table, beam, w_query, w_node, w_cross, bias_hidden, w_out):
    dma = pltpu.SemaphoreType.DMA
    scores = pl.pallas_call(
        kernel,
        out_shape=jax.ShapeDtypeStruct((COLS, Q), F32),
        in_specs=[pl.BlockSpec(memory_space=pl.ANY)] * 8,
        out_specs=pl.BlockSpec(memory_space=pltpu.VMEM),
        scratch_shapes=[
            pltpu.VMEM((Q, D), BF16),
            pltpu.VMEM((2 * PARENTS, D), BF16),
            pltpu.VMEM((Q, BEAM), I32),
            pltpu.VMEM((3, HID_DEV, D), BF16),
            pltpu.VMEM((1, HID_DEV), BF16),
            pltpu.VMEM((1, HID_DEV), BF16),
            pltpu.VMEM((HID, 4 * D), BF16),
            pltpu.VMEM((SERVED, Q, D), BF16),
            pltpu.VMEM((SERVED, 8, 128), F32),
            pltpu.VMEM((SERVED, 8, 128), F32),
            pltpu.VMEM((SERVED, 8, 128), F32),
            pltpu.VMEM((GROUPS, 8, 128), F32),
            pltpu.VMEM((2 * D, PARENTS), BF16),
            pltpu.VMEM((2 * PARENTS, D), F32),
            pltpu.VMEM((BEAM, BEAM), I32),
            pltpu.VMEM((Q, BEAM), I32),
            pltpu.VMEM((Q, BEAM), F32),
            pltpu.VMEM((Q, BEAM), F32),
            pltpu.VMEM((Q, BEAM), F32),
            pltpu.VMEM((Q, BEAM), F32),
            pltpu.VMEM((HID, 128), F32),
            pltpu.VMEM((HID, 128), F32),
            dma((8,)), dma((SERVED,)), dma((SERVED,)), dma((SERVED,)), dma((SERVED,)),
            dma((SHARES - 1,)), dma((SHARES - 1,)), dma((SERVED * SHARES,)), dma((GROUPS,)),
        ],
        compiler_params=pltpu.CompilerParams(collective_id=0, has_side_effects=True),
        name="beam_scores",
    )(
        queries, node_table, beam, w_query.T, w_node.T, w_cross.T,
        bias_hidden.reshape(1, HID_DEV), w_out.reshape(1, HID_DEV),
    )
    return scores.T


def solution(mesh):
    in_specs = (
        P("blk", None),
        P("blk", None),
        P("blk", None),
        P(None, "hid"),
        P(None, "hid"),
        P(None, "hid"),
        P("hid"),
        P("hid"),
    )
    return jax.shard_map(shards, mesh=mesh, in_specs=in_specs, out_specs=P("blk", "hid"), check_vma=False)
```

```python
import functools

import jax
import jax.numpy as jnp
from jax import lax
from jax.experimental import pallas as pl
from jax.experimental.pallas import tpu as pltpu
from jax.sharding import PartitionSpec as P

BF16, F32, I32 = jnp.bfloat16, jnp.float32, jnp.int32
RANK = jnp.int16
GROUPS = 32
SHARES = 4
SERVED = GROUPS // SHARES
Q = 96
BEAM = 128
D = 128
HID = 256
HID_DEV = HID // SHARES
PARENTS = 1024
ROWS = 3
SLOTS = ROWS * 128
COLS = BEAM // SHARES
STEP = 32
PAIR = 2
MESH = pl.DeviceIdType.MESH


def nt(a, b):
    return lax.dot_general(a, b, (((1,), (1,)), ((), ())), preferred_element_type=F32)


def nn(a, b):
    return jnp.dot(a, b, preferred_element_type=F32)


def iota(shape, dim):
    return lax.broadcasted_iota(I32, shape, dim)


def flag(cond):
    return jnp.where(cond, 1.0, 0.0).astype(BF16)


def eye(n):
    return flag(iota((n, n), 0) == iota((n, n), 1))


def wide_row(row, copies):
    return jnp.concatenate([jnp.broadcast_to(row, (16, row.shape[1])).astype(BF16)] * copies, axis=0)


def one_hot(row, height):
    row = wide_row(row, height // 16)
    match = iota((height, row.shape[1]), 0).astype(F32).astype(BF16) == row
    return jnp.where(match, jnp.ones(row.shape, BF16), jnp.zeros(row.shape, BF16))


def list_starts(owner, even, ids):
    lower = flag(iota((Q, Q), 0) > iota((Q, Q), 1))
    ones = jnp.ones((BEAM, BEAM), BF16)
    masks = [flag((owner == o) & even) for o in ids]
    before = nn(lower, jnp.concatenate(masks, axis=1))
    tall = [
        before[:, i * BEAM : (i + 1) * BEAM] - jnp.where((owner < o) & even, 1.0, 0.0) for i, o in enumerate(ids)
    ]
    total = nn(jnp.concatenate(tall, axis=0).astype(BF16), ones)
    picked = jnp.zeros((Q, BEAM), F32)
    for i, o in enumerate(ids):
        picked = jnp.where(owner == o, total[i * Q : (i + 1) * Q], picked)
    return picked.astype(I32)


def kernel(
    q_hbm, table_hbm, beam_hbm, wq_hbm, wn_hbm, wc_hbm, bias_hbm, wout_hbm, out_ref,
    q_ref, table_ref, beam_ref, w_in, bias_in, wout_in,
    w_all, qbuf, req, reqbuf, ret, retbuf, tt, t32, keys, inner, code_s, jl_s, a_s, b_s, wo_s, bi_s,
    in_sem, q_send, q_recv, r_send, r_recv, w_send, w_recv, s_send, s_recv,
):
    b, h = lax.axis_index("blk"), lax.axis_index("hid")
    y, xh, z = b // 8, (b // 4) % 2, b % 4
    xl, core = h // 2, h % 2
    my_place = (y // 2) * 4 + xh * 2 + z // 2
    flip = lax.rem(xh + xl + y, 2)
    own_zl = 1 - core

    def owner_of(i):
        return (i // 2) * 8 + lax.rem(flip + i // 2, 2) * 4 + lax.rem(i, 2) * 2 + own_zl

    def server_of(i):
        return lax.rem(y + i // 2, 2) * 2 + lax.rem(z, 2)

    def source_of(k):
        return ((k // 4) * 2 + lax.rem(xl + y, 2)) * 8 + ((k // 2) % 2) * 4 + (k % 2) * 2 + core

    loads = [
        pltpu.make_async_copy(src, dst, in_sem.at[n])
        for n, (src, dst) in enumerate((
            (beam_hbm, beam_ref), (wn_hbm, w_in.at[0]), (wc_hbm, w_in.at[1]), (wq_hbm, w_in.at[2]),
            (bias_hbm, bias_in), (wout_hbm, wout_in), (q_hbm, q_ref), (table_hbm, table_ref),
        ))
    ]
    for load in loads:
        load.start()

    barrier = pltpu.get_barrier_semaphore()
    served_self = z % 2 == h

    for k in range(SERVED):
        sender = lax.rem(xl + xh + (k // 2) % 2, 2) * 2 + 1 - z % 2
        pl.semaphore_signal(barrier, inc=1, device_id={"blk": source_of(k), "hid": sender}, device_id_type=MESH)

    for d in range(1, SHARES):
        pl.semaphore_signal(barrier, inc=1, device_id={"blk": b, "hid": (h + d) % SHARES}, device_id_type=MESH)

    for load in loads[:7]:
        load.wait()

    beam = beam_ref[...]
    even = (beam & 1) == 0
    owner = beam >> 11
    local = (beam >> 1) & (PARENTS - 1)
    tall = jnp.concatenate([beam, jnp.zeros((BEAM - Q, BEAM), I32)], axis=0).T
    parent = (tall >> 1).astype(RANK)
    keys[...] = jnp.where((tall & 1) == 0, tall >> 1, 32767)

    def count(step, acc):
        for u in range(16):
            row = jnp.broadcast_to(keys[pl.ds(16 * step + u, 1), :], (16, 128)).astype(RANK)
            row = jnp.concatenate([row] * 8, axis=0)
            acc = acc + jnp.where(row < parent, jnp.ones(acc.shape, RANK), jnp.zeros(acc.shape, RANK))
        return acc

    below = lax.fori_loop(0, BEAM // 16, count, jnp.zeros((BEAM, BEAM), RANK), unroll=False)
    below = below.astype(I32).T[:Q]
    inner[...] = below

    asked = (((owner >> 2) + (owner >> 3)) & 1 == flip) & ((owner & 1) == own_zl)
    group = jnp.where(asked, (owner >> 3) * 2 + ((owner >> 1) & 1), 64)
    rank = below + list_starts(owner, even, [owner_of(i) for i in range(SERVED)])
    code_s[...] = jnp.where(even & asked, group * 4 + (rank >> 7), 64).astype(F32)
    jl_s[...] = (rank & 127).astype(F32)
    a_s[...] = (local & 255).astype(F32)
    b_s[...] = (iota((Q, BEAM), 0) + 96 * (local >> 8) - 192).astype(F32)

    ident = eye(HID_DEV)
    vectors = jnp.concatenate(
        [jnp.broadcast_to(v[...].astype(F32), (64, HID_DEV)) for v in (bias_in, wout_in)], axis=0
    ).astype(BF16)
    my_rows = pl.ds(pl.multiple_of(h * HID_DEV, HID_DEV), HID_DEV)
    for n in range(3):
        w_all[my_rows, n * D : (n + 1) * D] = w_in[n]
    w_all[my_rows, 3 * D :] = nt(ident, vectors).astype(BF16)

    pl.semaphore_wait(barrier, SERVED + SHARES - 1)

    def q_copy(i):
        return pltpu.make_async_remote_copy(
            src_ref=q_ref, dst_ref=qbuf.at[my_place], send_sem=q_send.at[i], recv_sem=q_recv.at[my_place],
            device_id={"blk": owner_of(i), "hid": server_of(i)}, device_id_type=MESH,
        )

    def r_copy(i):
        return pltpu.make_async_remote_copy(
            src_ref=req.at[i], dst_ref=reqbuf.at[my_place], send_sem=r_send.at[i], recv_sem=r_recv.at[my_place],
            device_id={"blk": owner_of(i), "hid": server_of(i)}, device_id_type=MESH,
        )

    def w_copy(d):
        return pltpu.make_async_remote_copy(
            src_ref=w_all.at[my_rows], dst_ref=w_all.at[my_rows], send_sem=w_send.at[d - 1], recv_sem=w_recv.at[d - 1],
            device_id={"blk": b, "hid": (h + d) % SHARES}, device_id_type=MESH,
        )

    for d in range(1, SHARES):
        w_copy(d).start()

    def far(n):
        return lax.rem(y + 2 + n // 2, 4) * 2 + lax.rem(z // 2 + 1 + n, 2)

    @pl.loop(0, SERVED)
    def _(n):
        q_copy(far(n)).start()

    row64 = iota((64, BEAM), 0)
    target = ((row64 >> 3) * 4 + (row64 & 3)).astype(F32).astype(BF16)
    is_b = ((iota((16, BEAM), 0) >> 2) & 1).astype(F32).astype(BF16)
    is_a = 1 - is_b

    def compact(step, acc):
        values, places = [], []
        for u in range(STEP):
            at = pl.ds(STEP * step + u, 1)
            payload = is_a * wide_row(a_s[at, :], 1) + is_b * wide_row(b_s[at, :], 1)
            payload = jnp.concatenate([payload] * 4, axis=0)
            values.append(jnp.where(wide_row(code_s[at, :], 4) == target, payload, 0.0).astype(BF16))
            places.append(one_hot(jl_s[at, :], BEAM))
        return acc + nt(jnp.concatenate(values, axis=1), jnp.concatenate(places, axis=1))

    tables = lax.fori_loop(0, Q // STEP, compact, jnp.zeros((64, BEAM), F32), unroll=False)
    for i in range(SERVED):
        req[i] = tables[8 * i : 8 * i + 8].astype(BF16)

    @pl.loop(0, SERVED)
    def _(n):
        r_copy(far(n)).start()

    loads[7].wait()
    t32[...] = table_ref[...].astype(F32)
    ident = eye(D)
    for child in range(2):
        half = t32[pl.ds(child, PARENTS, stride=2), :].astype(BF16)
        tt[child * D : (child + 1) * D, :] = nt(ident, half).astype(BF16)

    def s_copy(k, d):
        return pltpu.make_async_remote_copy(
            src_ref=ret.at[k], dst_ref=retbuf.at[b], send_sem=s_send.at[k * SHARES + d], recv_sem=s_recv.at[b],
            device_id={"blk": source_of(k), "hid": d}, device_id_type=MESH,
        )

    def gather(places):
        asking, wanted = [], []
        for u, k in enumerate(places):
            digits = reqbuf[k].astype(F32)
            low, rest = digits[0:4], digits[4:8] + 192.0
            high = sum(jnp.where(rest >= 96.0 * n, 1.0, 0.0) for n in (1, 2, 3))
            rest = rest + (Q * u - 96.0 * high)
            low = low + 256.0 * high
            asking += [rest[r : r + 1] for r in range(ROWS)]
            wanted += [low[r : r + 1] for r in range(ROWS)]
        asking, wanted = jnp.concatenate(asking, axis=1), jnp.concatenate(wanted, axis=1)
        hot = jnp.concatenate([one_hot(wanted - 256.0 * c, 256) for c in range(PARENTS // 256)], axis=0)
        found = nn(tt[...], hot)
        queries = nt(eye(D), jnp.concatenate([qbuf[k] for k in places], axis=0)).astype(BF16)
        return found, nn(queries, one_hot(asking, Q * len(places)))

    def score(found, query):
        width = found.shape[1] // 128
        bias = jnp.concatenate([bi_s[...]] * width, axis=1)
        weight = jnp.concatenate([wo_s[...]] * width, axis=1)
        shared = nn(w_all[:, 2 * D : 3 * D], query.astype(BF16)) + bias
        totals = []
        for child in range(2):
            node = found[child * D : (child + 1) * D]
            joined = jnp.concatenate([node.astype(BF16), (node * query).astype(BF16)], axis=0)
            hidden = jnp.maximum(nn(w_all[:, : 2 * D], joined) + shared, 0.0)
            totals.append(jnp.sum(hidden * weight, axis=0, keepdims=True))
        scores = []
        for u in range(width // ROWS):
            rows = []
            for total in totals:
                rows += [total[:, r * 128 : (r + 1) * 128] for r in range(u * ROWS, (u + 1) * ROWS)]
                rows += [jnp.zeros((1, 128), F32)]
            scores.append(jnp.concatenate(rows, axis=0))
        return scores

    def near(n):
        a = lax.rem(y // 2 + n // 4, 2)
        e = lax.rem(xh + n, 2)
        return a * 4 + e * 2 + lax.rem(z // 2 + n // 2, 2)

    @pl.loop(0, SERVED // PAIR)
    def _(pair):
        places = [near(PAIR * pair + u) for u in range(PAIR)]
        for k in places:
            pltpu.make_async_remote_copy(
                src_ref=q_ref, dst_ref=qbuf.at[k], send_sem=q_send.at[k], recv_sem=q_recv.at[k],
                device_id={"blk": source_of(k), "hid": (h + 1) % SHARES}, device_id_type=MESH,
            ).wait_recv()
            pltpu.make_async_remote_copy(
                src_ref=req.at[k], dst_ref=reqbuf.at[k], send_sem=r_send.at[k], recv_sem=r_recv.at[k],
                device_id={"blk": source_of(k), "hid": (h + 1) % SHARES}, device_id_type=MESH,
            ).wait_recv()
        found, query = gather(places)

        @pl.when(pair == 0)
        def _():
            for d in range(1, SHARES):
                w_copy(d).wait_recv()
            bi_s[...] = jnp.broadcast_to(w_all[:, 3 * D : 3 * D + 1].astype(F32), (HID, 128))
            wo_s[...] = jnp.broadcast_to(w_all[:, 3 * D + 64 : 3 * D + 65].astype(F32), (HID, 128))

        for k, scores in zip(places, score(found, query)):
            ret[k] = scores
        for k in places:
            for d in range(SHARES):
                here = (d == h) & (source_of(k) == b)

                @pl.when(here)
                def _():
                    retbuf[b] = ret[k]

                @pl.when(jnp.logical_not(here))
                def _():
                    s_copy(k, d).start()

    def all_owners(g, acc):
        return acc + list_starts(owner, even, [g * SERVED + i for i in range(SERVED)])

    rank = lax.fori_loop(0, GROUPS // SERVED, all_owners, inner[...], unroll=False)
    code = owner * 4 + (rank >> 7)
    mine = flag(iota((COLS, BEAM), 1) == iota((COLS, BEAM), 0) + h * COLS)
    pad = jnp.zeros((BEAM - Q, BEAM), F32)

    def columns(values):
        return nt(mine, jnp.concatenate([values.astype(F32), pad], axis=0).astype(BF16))

    code_t, jl_t = columns(code), columns((beam & 1) * 128 + (rank & 127))

    @pl.loop(0, SERVED)
    def _(i):
        q_copy(i).wait_send()
        r_copy(i).wait_send()
        for d in range(SHARES):
            @pl.when(jnp.logical_not((d == h) & (source_of(i) == b)))
            def _():
                s_copy(i, d).wait_send()

    for d in range(1, SHARES):
        w_copy(d).wait_send()
    @pl.loop(0, GROUPS)
    def _(o):
        @pl.when(jnp.logical_not(served_self & (o == b)))
        def _():
            pltpu.make_async_remote_copy(
                src_ref=ret.at[0], dst_ref=retbuf.at[o], send_sem=s_send.at[0], recv_sem=s_recv.at[o],
                device_id={"blk": b, "hid": (h + 1) % SHARES}, device_id_type=MESH,
            ).wait_recv()

    table = jnp.concatenate(
        [retbuf[:, 4 * child : 4 * child + 4, :].reshape(GROUPS * 4, 128) for child in range(2)], axis=1
    )
    coarse = table.astype(BF16)
    parts = jnp.concatenate([coarse, (table - coarse.astype(F32)).astype(BF16)], axis=0)
    slot_row = iota((GROUPS * 4, 2 * 128), 0).astype(F32)
    for c in range(0, COLS, 2):
        hot = one_hot(jnp.concatenate([jl_t[c : c + 1], jl_t[c + 1 : c + 2]], axis=1), 256)
        which = jnp.concatenate([code_t[c : c + 1], code_t[c + 1 : c + 2]], axis=1)
        seen = nn(parts, hot)
        seen = seen[: GROUPS * 4] + seen[GROUPS * 4 :]
        total = jnp.sum(jnp.where(slot_row == which, seen, 0.0), axis=0, keepdims=True)
        out_ref[c : c + 1, :] = total[:, :Q]
        out_ref[c + 1 : c + 2, :] = total[:, 128 : 128 + Q]


def shards(queries, node_table, beam, w_query, w_node, w_cross, bias_hidden, w_out):
    dma = pltpu.SemaphoreType.DMA
    scores = pl.pallas_call(
        kernel,
        out_shape=jax.ShapeDtypeStruct((COLS, Q), F32),
        in_specs=[pl.BlockSpec(memory_space=pl.ANY)] * 8,
        out_specs=pl.BlockSpec(memory_space=pltpu.VMEM),
        scratch_shapes=[
            pltpu.VMEM((Q, D), BF16),
            pltpu.VMEM((2 * PARENTS, D), BF16),
            pltpu.VMEM((Q, BEAM), I32),
            pltpu.VMEM((3, HID_DEV, D), BF16),
            pltpu.VMEM((1, HID_DEV), BF16),
            pltpu.VMEM((1, HID_DEV), BF16),
            pltpu.VMEM((HID, 4 * D), BF16),
            pltpu.VMEM((SERVED, Q, D), BF16),
            pltpu.VMEM((SERVED, 8, 128), BF16),
            pltpu.VMEM((SERVED, 8, 128), BF16),
            pltpu.VMEM((SERVED, 8, 128), F32),
            pltpu.VMEM((GROUPS, 8, 128), F32),
            pltpu.VMEM((2 * D, PARENTS), BF16),
            pltpu.VMEM((2 * PARENTS, D), F32),
            pltpu.VMEM((BEAM, BEAM), I32),
            pltpu.VMEM((Q, BEAM), I32),
            pltpu.VMEM((Q, BEAM), F32),
            pltpu.VMEM((Q, BEAM), F32),
            pltpu.VMEM((Q, BEAM), F32),
            pltpu.VMEM((Q, BEAM), F32),
            pltpu.VMEM((HID, 128), F32),
            pltpu.VMEM((HID, 128), F32),
            dma((8,)), dma((SERVED,)), dma((SERVED,)), dma((SERVED,)), dma((SERVED,)),
            dma((SHARES - 1,)), dma((SHARES - 1,)), dma((SERVED * SHARES,)), dma((GROUPS,)),
        ],
        compiler_params=pltpu.CompilerParams(collective_id=0, has_side_effects=True),
        name="beam_scores",
    )(
        queries, node_table, beam, w_query.T, w_node.T, w_cross.T,
        bias_hidden.reshape(1, HID_DEV), w_out.reshape(1, HID_DEV),
    )
    return scores.T


def solution(mesh):
    in_specs = (
        P("blk", None),
        P("blk", None),
        P("blk", None),
        P(None, "hid"),
        P(None, "hid"),
        P(None, "hid"),
        P("hid"),
        P("hid"),
    )
    return jax.shard_map(shards, mesh=mesh, in_specs=in_specs, out_specs=P("blk", "hid"), check_vma=False)
```

```python
import functools

import jax
import jax.numpy as jnp
from jax import lax
from jax.experimental import pallas as pl
from jax.experimental.pallas import tpu as pltpu
from jax.sharding import PartitionSpec as P

BF16, F32, I32 = jnp.bfloat16, jnp.float32, jnp.int32
RANK = jnp.int16
GROUPS = 32
SHARES = 4
SERVED = GROUPS // SHARES
Q = 96
BEAM = 128
D = 128
HID = 256
HID_DEV = HID // SHARES
PARENTS = 1024
ROWS = 3
SLOTS = ROWS * 128
COLS = BEAM // SHARES
STEP = 32
PAIR = 2
MESH = pl.DeviceIdType.MESH


def nt(a, b):
    return lax.dot_general(a, b, (((1,), (1,)), ((), ())), preferred_element_type=F32)


def nn(a, b):
    return jnp.dot(a, b, preferred_element_type=F32)


def iota(shape, dim):
    return lax.broadcasted_iota(I32, shape, dim)


def flag(cond):
    return jnp.where(cond, 1.0, 0.0).astype(BF16)


def eye(n):
    return flag(iota((n, n), 0) == iota((n, n), 1))


def wide_row(row, copies):
    return jnp.concatenate([jnp.broadcast_to(row, (16, row.shape[1])).astype(BF16)] * copies, axis=0)


def one_hot(row, height):
    row = wide_row(row, height // 16)
    match = iota((height, row.shape[1]), 0).astype(F32).astype(BF16) == row
    return jnp.where(match, jnp.ones(row.shape, BF16), jnp.zeros(row.shape, BF16))


def list_starts(owner, even, ids):
    lower = flag(iota((Q, Q), 0) > iota((Q, Q), 1))
    ones = jnp.ones((BEAM, BEAM), BF16)
    masks = [flag((owner == o) & even) for o in ids]
    before = nn(lower, jnp.concatenate(masks, axis=1))
    tall = [
        before[:, i * BEAM : (i + 1) * BEAM] - jnp.where((owner < o) & even, 1.0, 0.0) for i, o in enumerate(ids)
    ]
    total = nn(jnp.concatenate(tall, axis=0).astype(BF16), ones)
    picked = jnp.zeros((Q, BEAM), F32)
    for i, o in enumerate(ids):
        picked = jnp.where(owner == o, total[i * Q : (i + 1) * Q], picked)
    return picked.astype(I32)


def kernel(
    q_hbm, table_hbm, beam_hbm, wq_hbm, wn_hbm, wc_hbm, bias_hbm, wout_hbm, out_ref,
    q_ref, table_ref, beam_ref, w_in, bias_in, wout_in,
    w_all, qbuf, req, reqbuf, ret, retbuf, tt, t32, keys, inner, code_s, jl_s, a_s, b_s, wo_s, bi_s,
    in_sem, q_send, q_recv, r_send, r_recv, w_send, w_recv, s_send, s_recv,
):
    b, h = lax.axis_index("blk"), lax.axis_index("hid")
    y, xh, z = b // 8, (b // 4) % 2, b % 4
    xl, core = h // 2, h % 2
    my_place = (y // 2) * 4 + xh * 2 + z // 2
    flip = lax.rem(xh + xl + y, 2)
    own_zl = 1 - core

    def owner_of(i):
        return (i // 2) * 8 + lax.rem(flip + i // 2, 2) * 4 + lax.rem(i, 2) * 2 + own_zl

    def server_of(i):
        return lax.rem(y + i // 2, 2) * 2 + lax.rem(z, 2)

    def source_of(k):
        return ((k // 4) * 2 + lax.rem(xl + y, 2)) * 8 + ((k // 2) % 2) * 4 + (k % 2) * 2 + core

    loads = [
        pltpu.make_async_copy(src, dst, in_sem.at[n])
        for n, (src, dst) in enumerate((
            (beam_hbm, beam_ref), (wn_hbm, w_in.at[0]), (wc_hbm, w_in.at[1]), (wq_hbm, w_in.at[2]),
            (bias_hbm, bias_in), (wout_hbm, wout_in), (q_hbm, q_ref), (table_hbm, table_ref),
        ))
    ]
    for load in loads:
        load.start()

    barrier = pltpu.get_barrier_semaphore()
    served_self = z % 2 == h

    for k in range(SERVED):
        sender = lax.rem(xl + xh + (k // 2) % 2, 2) * 2 + 1 - z % 2
        pl.semaphore_signal(barrier, inc=1, device_id={"blk": source_of(k), "hid": sender}, device_id_type=MESH)

    for d in range(1, SHARES):
        pl.semaphore_signal(barrier, inc=1, device_id={"blk": b, "hid": (h + d) % SHARES}, device_id_type=MESH)

    for load in loads[:7]:
        load.wait()

    beam = beam_ref[...]
    even = (beam & 1) == 0
    owner = beam >> 11
    local = (beam >> 1) & (PARENTS - 1)
    tall = jnp.concatenate([beam, jnp.zeros((BEAM - Q, BEAM), I32)], axis=0).T
    parent = (tall >> 1).astype(RANK)
    keys[...] = jnp.where((tall & 1) == 0, tall >> 1, 32767)

    def count(step, acc):
        for u in range(16):
            row = jnp.broadcast_to(keys[pl.ds(16 * step + u, 1), :], (16, 128)).astype(RANK)
            row = jnp.concatenate([row] * 8, axis=0)
            acc = acc + jnp.where(row < parent, jnp.ones(acc.shape, RANK), jnp.zeros(acc.shape, RANK))
        return acc

    below = lax.fori_loop(0, BEAM // 16, count, jnp.zeros((BEAM, BEAM), RANK), unroll=False)
    below = below.astype(I32).T[:Q]
    inner[...] = below

    asked = (((owner >> 2) + (owner >> 3)) & 1 == flip) & ((owner & 1) == own_zl)
    group = jnp.where(asked, (owner >> 3) * 2 + ((owner >> 1) & 1), 64)
    rank = below + list_starts(owner, even, [owner_of(i) for i in range(SERVED)])
    code_s[...] = jnp.where(even & asked, group * 4 + (rank >> 7), 64).astype(F32)
    jl_s[...] = (rank & 127).astype(F32)
    a_s[...] = (local & 255).astype(F32)
    b_s[...] = (iota((Q, BEAM), 0) + 96 * (local >> 8) - 192).astype(F32)

    ident = eye(HID_DEV)
    vectors = jnp.concatenate(
        [jnp.broadcast_to(v[...].astype(F32), (64, HID_DEV)) for v in (bias_in, wout_in)], axis=0
    ).astype(BF16)
    my_rows = pl.ds(pl.multiple_of(h * HID_DEV, HID_DEV), HID_DEV)
    for n in range(3):
        w_all[my_rows, n * D : (n + 1) * D] = w_in[n]
    w_all[my_rows, 3 * D :] = nt(ident, vectors).astype(BF16)

    pl.semaphore_wait(barrier, SERVED + SHARES - 1)

    def all_of(ref, send_sem, recv_sem):
        return pltpu.make_async_remote_copy(
            src_ref=ref, dst_ref=ref, send_sem=send_sem, recv_sem=recv_sem,
            device_id={"blk": b, "hid": (h + 1) % SHARES}, device_id_type=MESH,
        )

    def q_copy(i):
        return pltpu.make_async_remote_copy(
            src_ref=q_ref, dst_ref=qbuf.at[my_place], send_sem=q_send, recv_sem=q_recv.at[my_place],
            device_id={"blk": owner_of(i), "hid": server_of(i)}, device_id_type=MESH,
        )

    def r_copy(i):
        return pltpu.make_async_remote_copy(
            src_ref=req.at[i], dst_ref=reqbuf.at[my_place], send_sem=r_send, recv_sem=r_recv.at[my_place],
            device_id={"blk": owner_of(i), "hid": server_of(i)}, device_id_type=MESH,
        )

    def w_copy(d):
        return pltpu.make_async_remote_copy(
            src_ref=w_all.at[my_rows], dst_ref=w_all.at[my_rows], send_sem=w_send, recv_sem=w_recv,
            device_id={"blk": b, "hid": (h + d) % SHARES}, device_id_type=MESH,
        )

    for d in range(1, SHARES):
        w_copy(d).start()

    def far(n):
        return lax.rem(y + 2 + n // 2, 4) * 2 + lax.rem(z // 2 + 1 + n, 2)

    @pl.loop(0, SERVED)
    def _(n):
        q_copy(far(n)).start()

    row64 = iota((64, BEAM), 0)
    target = ((row64 >> 3) * 4 + (row64 & 3)).astype(F32).astype(BF16)
    is_b = ((iota((16, BEAM), 0) >> 2) & 1).astype(F32).astype(BF16)
    is_a = 1 - is_b

    def compact(step, acc):
        values, places = [], []
        for u in range(STEP):
            at = pl.ds(STEP * step + u, 1)
            payload = is_a * wide_row(a_s[at, :], 1) + is_b * wide_row(b_s[at, :], 1)
            payload = jnp.concatenate([payload] * 4, axis=0)
            values.append(jnp.where(wide_row(code_s[at, :], 4) == target, payload, 0.0).astype(BF16))
            places.append(one_hot(jl_s[at, :], BEAM))
        return acc + nt(jnp.concatenate(values, axis=1), jnp.concatenate(places, axis=1))

    tables = lax.fori_loop(0, Q // STEP, compact, jnp.zeros((64, BEAM), F32), unroll=False)
    for i in range(SERVED):
        req[i] = tables[8 * i : 8 * i + 8].astype(BF16)

    @pl.loop(0, SERVED)
    def _(n):
        r_copy(far(n)).start()

    loads[7].wait()
    t32[...] = table_ref[...].astype(F32)
    ident = eye(D)
    for child in range(2):
        half = t32[pl.ds(child, PARENTS, stride=2), :].astype(BF16)
        tt[child * D : (child + 1) * D, :] = nt(ident, half).astype(BF16)

    def s_copy(k, d):
        return pltpu.make_async_remote_copy(
            src_ref=ret.at[k], dst_ref=retbuf.at[b], send_sem=s_send, recv_sem=s_recv,
            device_id={"blk": source_of(k), "hid": d}, device_id_type=MESH,
        )

    def gather(places):
        asking, wanted = [], []
        for u, k in enumerate(places):
            digits = reqbuf[k].astype(F32)
            low, rest = digits[0:4], digits[4:8] + 192.0
            high = sum(jnp.where(rest >= 96.0 * n, 1.0, 0.0) for n in (1, 2, 3))
            rest = rest + (Q * u - 96.0 * high)
            low = low + 256.0 * high
            asking += [rest[r : r + 1] for r in range(ROWS)]
            wanted += [low[r : r + 1] for r in range(ROWS)]
        asking, wanted = jnp.concatenate(asking, axis=1), jnp.concatenate(wanted, axis=1)
        hot = jnp.concatenate([one_hot(wanted - 256.0 * c, 256) for c in range(PARENTS // 256)], axis=0)
        found = nn(tt[...], hot)
        queries = nt(eye(D), jnp.concatenate([qbuf[k] for k in places], axis=0)).astype(BF16)
        return found, nn(queries, one_hot(asking, Q * len(places)))

    def score(found, query):
        width = found.shape[1] // 128
        bias = jnp.concatenate([bi_s[...]] * width, axis=1)
        weight = jnp.concatenate([wo_s[...]] * width, axis=1)
        shared = nn(w_all[:, 2 * D : 3 * D], query.astype(BF16)) + bias
        totals = []
        for child in range(2):
            node = found[child * D : (child + 1) * D]
            joined = jnp.concatenate([node.astype(BF16), (node * query).astype(BF16)], axis=0)
            hidden = jnp.maximum(nn(w_all[:, : 2 * D], joined) + shared, 0.0)
            totals.append(jnp.sum(hidden * weight, axis=0, keepdims=True))
        scores = []
        for u in range(width // ROWS):
            rows = []
            for total in totals:
                rows += [total[:, r * 128 : (r + 1) * 128] for r in range(u * ROWS, (u + 1) * ROWS)]
                rows += [jnp.zeros((1, 128), F32)]
            scores.append(jnp.concatenate(rows, axis=0))
        return scores

    def near(n):
        a = lax.rem(y // 2 + n // 4, 2)
        e = lax.rem(xh + n, 2)
        return a * 4 + e * 2 + lax.rem(z // 2 + n // 2, 2)

    @pl.loop(0, SERVED // PAIR)
    def _(pair):
        places = [near(PAIR * pair + u) for u in range(PAIR)]
        for k in places:
            pltpu.make_async_remote_copy(
                src_ref=q_ref, dst_ref=qbuf.at[k], send_sem=q_send, recv_sem=q_recv.at[k],
                device_id={"blk": source_of(k), "hid": (h + 1) % SHARES}, device_id_type=MESH,
            ).wait_recv()
            pltpu.make_async_remote_copy(
                src_ref=req.at[k], dst_ref=reqbuf.at[k], send_sem=r_send, recv_sem=r_recv.at[k],
                device_id={"blk": source_of(k), "hid": (h + 1) % SHARES}, device_id_type=MESH,
            ).wait_recv()
        found, query = gather(places)

        @pl.when(pair == 0)
        def _():
            all_of(w_all.at[: HID - HID_DEV], w_send, w_recv).wait_recv()
            bi_s[...] = jnp.broadcast_to(w_all[:, 3 * D : 3 * D + 1].astype(F32), (HID, 128))
            wo_s[...] = jnp.broadcast_to(w_all[:, 3 * D + 64 : 3 * D + 65].astype(F32), (HID, 128))

        for k, scores in zip(places, score(found, query)):
            ret[k] = scores
        for k in places:
            for d in range(SHARES):
                here = (d == h) & (source_of(k) == b)

                @pl.when(here)
                def _():
                    retbuf[b] = ret[k]

                @pl.when(jnp.logical_not(here))
                def _():
                    s_copy(k, d).start()

    def all_owners(g, acc):
        return acc + list_starts(owner, even, [g * SERVED + i for i in range(SERVED)])

    rank = lax.fori_loop(0, GROUPS // SERVED, all_owners, inner[...], unroll=False)
    code = owner * 4 + (rank >> 7)
    mine = flag(iota((COLS, BEAM), 1) == iota((COLS, BEAM), 0) + h * COLS)
    pad = jnp.zeros((BEAM - Q, BEAM), F32)

    def columns(values):
        return nt(mine, jnp.concatenate([values.astype(F32), pad], axis=0).astype(BF16))

    code_t, jl_t = columns(code), columns((beam & 1) * 128 + (rank & 127))

    all_of(qbuf, q_send, q_recv.at[0]).wait_send()
    all_of(reqbuf, r_send, r_recv.at[0]).wait_send()
    all_of(w_all.at[: HID - HID_DEV], w_send, w_recv).wait_send()

    @pl.when(served_self)
    def _():
        all_of(retbuf.at[: GROUPS - 1], s_send, s_recv).wait_send()

    @pl.when(jnp.logical_not(served_self))
    def _():
        all_of(retbuf, s_send, s_recv).wait_send()

    @pl.when(served_self)
    def _():
        all_of(retbuf.at[: GROUPS - 1], s_send, s_recv).wait_recv()

    @pl.when(jnp.logical_not(served_self))
    def _():
        all_of(retbuf, s_send, s_recv).wait_recv()

    table = jnp.concatenate(
        [retbuf[:, 4 * child : 4 * child + 4, :].reshape(GROUPS * 4, 128) for child in range(2)], axis=1
    )
    coarse = table.astype(BF16)
    parts = jnp.concatenate([coarse, (table - coarse.astype(F32)).astype(BF16)], axis=0)
    slot_row = iota((GROUPS * 4, 2 * 128), 0).astype(F32)
    for c in range(0, COLS, 2):
        hot = one_hot(jnp.concatenate([jl_t[c : c + 1], jl_t[c + 1 : c + 2]], axis=1), 256)
        which = jnp.concatenate([code_t[c : c + 1], code_t[c + 1 : c + 2]], axis=1)
        seen = nn(parts, hot)
        seen = seen[: GROUPS * 4] + seen[GROUPS * 4 :]
        total = jnp.sum(jnp.where(slot_row == which, seen, 0.0), axis=0, keepdims=True)
        out_ref[c : c + 1, :] = total[:, :Q]
        out_ref[c + 1 : c + 2, :] = total[:, 128 : 128 + Q]


def shards(queries, node_table, beam, w_query, w_node, w_cross, bias_hidden, w_out):
    dma = pltpu.SemaphoreType.DMA
    scores = pl.pallas_call(
        kernel,
        out_shape=jax.ShapeDtypeStruct((COLS, Q), F32),
        in_specs=[pl.BlockSpec(memory_space=pl.ANY)] * 8,
        out_specs=pl.BlockSpec(memory_space=pltpu.VMEM),
        scratch_shapes=[
            pltpu.VMEM((Q, D), BF16),
            pltpu.VMEM((2 * PARENTS, D), BF16),
            pltpu.VMEM((Q, BEAM), I32),
            pltpu.VMEM((3, HID_DEV, D), BF16),
            pltpu.VMEM((1, HID_DEV), BF16),
            pltpu.VMEM((1, HID_DEV), BF16),
            pltpu.VMEM((HID, 4 * D), BF16),
            pltpu.VMEM((SERVED, Q, D), BF16),
            pltpu.VMEM((SERVED, 8, 128), BF16),
            pltpu.VMEM((SERVED, 8, 128), BF16),
            pltpu.VMEM((SERVED, 8, 128), F32),
            pltpu.VMEM((GROUPS, 8, 128), F32),
            pltpu.VMEM((2 * D, PARENTS), BF16),
            pltpu.VMEM((2 * PARENTS, D), F32),
            pltpu.VMEM((BEAM, BEAM), I32),
            pltpu.VMEM((Q, BEAM), I32),
            pltpu.VMEM((Q, BEAM), F32),
            pltpu.VMEM((Q, BEAM), F32),
            pltpu.VMEM((Q, BEAM), F32),
            pltpu.VMEM((Q, BEAM), F32),
            pltpu.VMEM((HID, 128), F32),
            pltpu.VMEM((HID, 128), F32),
            dma((8,)), dma(()), dma((SERVED,)), dma(()), dma((SERVED,)), dma(()), dma(()), dma(()), dma(()),
        ],
        compiler_params=pltpu.CompilerParams(collective_id=0, has_side_effects=True, vmem_limit_bytes=16 << 20),
        name="beam_scores",
    )(*[pltpu.with_memory_space_constraint(x, pltpu.HBM) for x in (
        queries, node_table, beam, w_query.T, w_node.T, w_cross.T,
        bias_hidden.reshape(1, HID_DEV), w_out.reshape(1, HID_DEV),
    )])
    return scores.T


def solution(mesh):
    in_specs = (
        P("blk", None),
        P("blk", None),
        P("blk", None),
        P(None, "hid"),
        P(None, "hid"),
        P(None, "hid"),
        P("hid"),
        P("hid"),
    )
    return jax.shard_map(shards, mesh=mesh, in_specs=in_specs, out_specs=P("blk", "hid"), check_vma=False)
```

```python
import functools

import jax
import jax.numpy as jnp
from jax import lax
from jax.experimental import pallas as pl
from jax.experimental.pallas import tpu as pltpu
from jax.sharding import PartitionSpec as P

BF16, F32, I32 = jnp.bfloat16, jnp.float32, jnp.int32
RANK = jnp.int16
GROUPS = 32
SHARES = 4
SERVED = GROUPS // SHARES
Q = 96
BEAM = 128
D = 128
HID = 256
HID_DEV = HID // SHARES
PARENTS = 1024
ROWS = 3
SLOTS = ROWS * 128
COLS = BEAM // SHARES
STEP = 32
PAIR = 2
MESH = pl.DeviceIdType.MESH


def nt(a, b):
    return lax.dot_general(a, b, (((1,), (1,)), ((), ())), preferred_element_type=F32)


def nn(a, b):
    return jnp.dot(a, b, preferred_element_type=F32)


def iota(shape, dim):
    return lax.broadcasted_iota(I32, shape, dim)


def flag(cond):
    return jnp.where(cond, 1.0, 0.0).astype(BF16)


def eye(n):
    return flag(iota((n, n), 0) == iota((n, n), 1))


def wide_row(row, copies):
    return jnp.concatenate([jnp.broadcast_to(row, (16, row.shape[1])).astype(BF16)] * copies, axis=0)


def one_hot(row, height):
    row = wide_row(row, height // 16)
    match = iota((height, row.shape[1]), 0).astype(F32).astype(BF16) == row
    return jnp.where(match, jnp.ones(row.shape, BF16), jnp.zeros(row.shape, BF16))


def list_starts(owner, even, ids):
    lower = flag(iota((Q, Q), 0) > iota((Q, Q), 1))
    ones = jnp.ones((BEAM, BEAM), BF16)
    masks = [flag((owner == o) & even) for o in ids]
    before = nn(lower, jnp.concatenate(masks, axis=1))
    tall = [
        before[:, i * BEAM : (i + 1) * BEAM] - jnp.where((owner < o) & even, 1.0, 0.0) for i, o in enumerate(ids)
    ]
    total = nn(jnp.concatenate(tall, axis=0).astype(BF16), ones)
    picked = jnp.zeros((Q, BEAM), F32)
    for i, o in enumerate(ids):
        picked = jnp.where(owner == o, total[i * Q : (i + 1) * Q], picked)
    return picked.astype(I32)


def kernel(
    q_hbm, table_hbm, beam_hbm, wq_hbm, wn_hbm, wc_hbm, bias_hbm, wout_hbm, out_ref,
    q_ref, table_ref, beam_ref, w_in, bias_in, wout_in,
    w_all, qbuf, req, reqbuf, ret, retbuf, tt, t32, keys, inner, code_s, jl_s, a_s, b_s, wo_s, joined,
    in_sem, q_send, q_recv, r_send, r_recv, w_send, w_recv, s_send, s_recv,
):
    b, h = lax.axis_index("blk"), lax.axis_index("hid")
    y, xh, z = b // 8, (b // 4) % 2, b % 4
    xl, core = h // 2, h % 2
    my_place = (y // 2) * 4 + xh * 2 + z // 2
    flip = lax.rem(xh + xl + y, 2)
    own_zl = 1 - core

    def owner_of(i):
        return (i // 2) * 8 + lax.rem(flip + i // 2, 2) * 4 + lax.rem(i, 2) * 2 + own_zl

    def server_of(i):
        return lax.rem(y + i // 2, 2) * 2 + lax.rem(z, 2)

    def source_of(k):
        return ((k // 4) * 2 + lax.rem(xl + y, 2)) * 8 + ((k // 2) % 2) * 4 + (k % 2) * 2 + core

    loads = [
        pltpu.make_async_copy(src, dst, in_sem.at[n])
        for n, (src, dst) in enumerate((
            (beam_hbm, beam_ref), (wn_hbm, w_in.at[0]), (wc_hbm, w_in.at[1]), (wq_hbm, w_in.at[2]),
            (bias_hbm, bias_in), (wout_hbm, wout_in), (q_hbm, q_ref), (table_hbm, table_ref),
        ))
    ]
    for load in loads:
        load.start()

    barrier = pltpu.get_barrier_semaphore()
    served_self = z % 2 == h

    for k in range(SERVED):
        sender = lax.rem(xl + xh + (k // 2) % 2, 2) * 2 + 1 - z % 2
        pl.semaphore_signal(barrier, inc=1, device_id={"blk": source_of(k), "hid": sender}, device_id_type=MESH)

    for d in range(1, SHARES):
        pl.semaphore_signal(barrier, inc=1, device_id={"blk": b, "hid": (h + d) % SHARES}, device_id_type=MESH)

    for load in loads[:7]:
        load.wait()

    beam = beam_ref[...]
    even = (beam & 1) == 0
    owner = beam >> 11
    local = (beam >> 1) & (PARENTS - 1)
    tall = jnp.concatenate([beam, jnp.zeros((BEAM - Q, BEAM), I32)], axis=0).T
    parent = (tall >> 1).astype(RANK)
    keys[...] = jnp.where((tall & 1) == 0, tall >> 1, 32767)

    def count(step, acc):
        for u in range(16):
            row = jnp.broadcast_to(keys[pl.ds(16 * step + u, 1), :], (16, 128)).astype(RANK)
            row = jnp.concatenate([row] * 8, axis=0)
            acc = acc + jnp.where(row < parent, jnp.ones(acc.shape, RANK), jnp.zeros(acc.shape, RANK))
        return acc

    below = lax.fori_loop(0, BEAM // 16, count, jnp.zeros((BEAM, BEAM), RANK), unroll=False)
    below = below.astype(I32).T[:Q]
    inner[...] = below

    asked = (((owner >> 2) + (owner >> 3)) & 1 == flip) & ((owner & 1) == own_zl)
    group = jnp.where(asked, (owner >> 3) * 2 + ((owner >> 1) & 1), 64)
    rank = below + list_starts(owner, even, [owner_of(i) for i in range(SERVED)])
    code_s[...] = jnp.where(even & asked, group * 4 + (rank >> 7), 64).astype(F32)
    jl_s[...] = (rank & 127).astype(F32)
    a_s[...] = (local & 255).astype(F32)
    b_s[...] = (iota((Q, BEAM), 0) + 96 * (local >> 8) - 192).astype(F32)

    ident = eye(HID_DEV)
    vectors = jnp.concatenate(
        [jnp.broadcast_to(v[...].astype(F32), (64, HID_DEV)) for v in (bias_in, wout_in)], axis=0
    ).astype(BF16)
    my_rows = pl.ds(pl.multiple_of(h * HID_DEV, HID_DEV), HID_DEV)
    for n in range(3):
        w_all[my_rows, n * D : (n + 1) * D] = w_in[n]
    w_all[my_rows, 3 * D :] = nt(ident, vectors).astype(BF16)

    row64 = iota((64, BEAM), 0)
    target = ((row64 >> 3) * 4 + (row64 & 3)).astype(F32).astype(BF16)
    is_b = ((iota((16, BEAM), 0) >> 2) & 1).astype(F32).astype(BF16)
    is_a = 1 - is_b

    def compact(step, acc):
        values, places = [], []
        for u in range(STEP):
            at = pl.ds(STEP * step + u, 1)
            payload = is_a * wide_row(a_s[at, :], 1) + is_b * wide_row(b_s[at, :], 1)
            payload = jnp.concatenate([payload] * 4, axis=0)
            values.append(jnp.where(wide_row(code_s[at, :], 4) == target, payload, 0.0).astype(BF16))
            places.append(one_hot(jl_s[at, :], BEAM))
        return acc + nt(jnp.concatenate(values, axis=1), jnp.concatenate(places, axis=1))

    tables = lax.fori_loop(0, Q // STEP, compact, jnp.zeros((64, BEAM), F32), unroll=False)
    for i in range(SERVED):
        req[i] = tables[8 * i : 8 * i + 8].astype(BF16)

    pl.semaphore_wait(barrier, SERVED + SHARES - 1)

    def all_of(ref, send_sem, recv_sem):
        return pltpu.make_async_remote_copy(
            src_ref=ref, dst_ref=ref, send_sem=send_sem, recv_sem=recv_sem,
            device_id={"blk": b, "hid": (h + 1) % SHARES}, device_id_type=MESH,
        )

    def q_copy(i):
        return pltpu.make_async_remote_copy(
            src_ref=q_ref, dst_ref=qbuf.at[my_place], send_sem=q_send, recv_sem=q_recv.at[my_place],
            device_id={"blk": owner_of(i), "hid": server_of(i)}, device_id_type=MESH,
        )

    def r_copy(i):
        return pltpu.make_async_remote_copy(
            src_ref=req.at[i], dst_ref=reqbuf.at[my_place], send_sem=r_send, recv_sem=r_recv.at[my_place],
            device_id={"blk": owner_of(i), "hid": server_of(i)}, device_id_type=MESH,
        )

    def w_copy(d):
        return pltpu.make_async_remote_copy(
            src_ref=w_all.at[my_rows], dst_ref=w_all.at[my_rows], send_sem=w_send, recv_sem=w_recv,
            device_id={"blk": b, "hid": (h + d) % SHARES}, device_id_type=MESH,
        )

    for d in range(1, SHARES):
        w_copy(d).start()

    def far(n):
        return lax.rem(y + 2 + n // 2, 4) * 2 + lax.rem(z // 2 + 1 + n, 2)

    @pl.loop(0, SERVED)
    def _(n):
        r_copy(far(n)).start()
        q_copy(far(n)).start()

    loads[7].wait()
    t32[...] = table_ref[...].astype(F32)
    ident = eye(D)
    for child in range(2):
        half = t32[pl.ds(child, PARENTS, stride=2), :].astype(BF16)
        tt[child * D : (child + 1) * D, :] = nt(ident, half).astype(BF16)

    one_row = flag(iota((D, PAIR * SLOTS), 0) == 0)
    for slot in range(2):
        joined[slot, 5 * D :] = one_row

    def s_copy(k, d):
        return pltpu.make_async_remote_copy(
            src_ref=ret.at[k], dst_ref=retbuf.at[b], send_sem=s_send, recv_sem=s_recv,
            device_id={"blk": source_of(k), "hid": d}, device_id_type=MESH,
        )

    def gather(places, slot):
        asking, wanted = [], []
        for u, k in enumerate(places):
            digits = reqbuf[k].astype(F32)
            low, rest = digits[0:4], digits[4:8] + 192.0
            high = sum(jnp.where(rest >= 96.0 * n, 1.0, 0.0) for n in (1, 2, 3))
            rest = rest + (Q * u - 96.0 * high)
            low = low + 256.0 * high
            asking += [rest[r : r + 1] for r in range(ROWS)]
            wanted += [low[r : r + 1] for r in range(ROWS)]
        asking, wanted = jnp.concatenate(asking, axis=1), jnp.concatenate(wanted, axis=1)
        hot = jnp.concatenate([one_hot(wanted - 256.0 * c, 256) for c in range(PARENTS // 256)], axis=0)
        found = nn(tt[...], hot)
        queries = nt(eye(D), jnp.concatenate([qbuf[k] for k in places], axis=0)).astype(BF16)
        query = nn(queries, one_hot(asking, Q * len(places)))
        for child in range(2):
            node = found[child * D : (child + 1) * D]
            joined[slot, 2 * child * D : (2 * child + 1) * D] = node.astype(BF16)
            joined[slot, (2 * child + 1) * D : (2 * child + 2) * D] = (node * query).astype(BF16)
        joined[slot, 4 * D : 5 * D] = query.astype(BF16)

    def score(slot):
        width = joined.shape[2] // 128
        weight = jnp.concatenate([wo_s[...]] * width, axis=1)
        shared = nn(w_all[:, 2 * D :], joined[slot, 4 * D : 6 * D])
        totals = []
        for child in range(2):
            hidden = jnp.maximum(nn(w_all[:, : 2 * D], joined[slot, 2 * child * D : 2 * (child + 1) * D]) + shared, 0.0)
            totals.append(jnp.sum(hidden * weight, axis=0, keepdims=True))
        scores = []
        for u in range(width // ROWS):
            rows = []
            for total in totals:
                rows += [total[:, r * 128 : (r + 1) * 128] for r in range(u * ROWS, (u + 1) * ROWS)]
                rows += [jnp.zeros((1, 128), F32)]
            scores.append(jnp.concatenate(rows, axis=0))
        return scores

    def near(n):
        a = lax.rem(y // 2 + n // 4, 2)
        e = lax.rem(xh + n, 2)
        return a * 4 + e * 2 + lax.rem(z // 2 + n // 2, 2)

    def arrive(places):
        for k in places:
            pltpu.make_async_remote_copy(
                src_ref=q_ref, dst_ref=qbuf.at[k], send_sem=q_send, recv_sem=q_recv.at[k],
                device_id={"blk": source_of(k), "hid": (h + 1) % SHARES}, device_id_type=MESH,
            ).wait_recv()
            pltpu.make_async_remote_copy(
                src_ref=req.at[k], dst_ref=reqbuf.at[k], send_sem=r_send, recv_sem=r_recv.at[k],
                device_id={"blk": source_of(k), "hid": (h + 1) % SHARES}, device_id_type=MESH,
            ).wait_recv()

    steps = [[near(PAIR * pair + u) for u in range(PAIR)] for pair in range(SERVED // PAIR)]
    arrive(steps[0])
    gather(steps[0], 0)
    all_of(w_all.at[: HID - HID_DEV], w_send, w_recv).wait_recv()
    wo_s[...] = jnp.broadcast_to(w_all[:, 3 * D + 64 : 3 * D + 65].astype(F32), (HID, 128))
    for pair, places in enumerate(steps):
        if pair + 1 < len(steps):
            arrive(steps[pair + 1])
        for k, scores in zip(places, score(pair % 2)):
            ret[k] = scores
        if pair + 1 < len(steps):
            gather(steps[pair + 1], (pair + 1) % 2)
        for k in places:
            for d in range(SHARES):
                here = (d == h) & (source_of(k) == b)

                @pl.when(here)
                def _():
                    retbuf[b] = ret[k]

                @pl.when(jnp.logical_not(here))
                def _():
                    s_copy(k, d).start()

    def all_owners(g, acc):
        return acc + list_starts(owner, even, [g * SERVED + i for i in range(SERVED)])

    rank = lax.fori_loop(0, GROUPS // SERVED, all_owners, inner[...], unroll=False)
    code = owner * 4 + (rank >> 7)
    mine = flag(iota((COLS, BEAM), 1) == iota((COLS, BEAM), 0) + h * COLS)
    pad = jnp.zeros((BEAM - Q, BEAM), F32)

    def columns(values):
        return nt(mine, jnp.concatenate([values.astype(F32), pad], axis=0).astype(BF16))

    code_t, jl_t = columns(code), columns((beam & 1) * 128 + (rank & 127))

    all_of(qbuf, q_send, q_recv.at[0]).wait_send()
    all_of(reqbuf, r_send, r_recv.at[0]).wait_send()
    all_of(w_all.at[: HID - HID_DEV], w_send, w_recv).wait_send()

    @pl.when(served_self)
    def _():
        all_of(retbuf.at[: GROUPS - 1], s_send, s_recv).wait_send()

    @pl.when(jnp.logical_not(served_self))
    def _():
        all_of(retbuf, s_send, s_recv).wait_send()

    @pl.when(served_self)
    def _():
        all_of(retbuf.at[: GROUPS - 1], s_send, s_recv).wait_recv()

    @pl.when(jnp.logical_not(served_self))
    def _():
        all_of(retbuf, s_send, s_recv).wait_recv()

    table = jnp.concatenate(
        [retbuf[:, 4 * child : 4 * child + 4, :].reshape(GROUPS * 4, 128) for child in range(2)], axis=1
    )
    coarse = table.astype(BF16)
    parts = jnp.concatenate([coarse, (table - coarse.astype(F32)).astype(BF16)], axis=0)
    slot_row = iota((GROUPS * 4, 2 * 128), 0).astype(F32)
    for c in range(0, COLS, 2):
        hot = one_hot(jnp.concatenate([jl_t[c : c + 1], jl_t[c + 1 : c + 2]], axis=1), 256)
        which = jnp.concatenate([code_t[c : c + 1], code_t[c + 1 : c + 2]], axis=1)
        seen = nn(parts, hot)
        seen = seen[: GROUPS * 4] + seen[GROUPS * 4 :]
        total = jnp.sum(jnp.where(slot_row == which, seen, 0.0), axis=0, keepdims=True)
        out_ref[c : c + 1, :] = total[:, :Q]
        out_ref[c + 1 : c + 2, :] = total[:, 128 : 128 + Q]


def shards(queries, node_table, beam, w_query, w_node, w_cross, bias_hidden, w_out):
    dma = pltpu.SemaphoreType.DMA
    scores = pl.pallas_call(
        kernel,
        out_shape=jax.ShapeDtypeStruct((COLS, Q), F32),
        in_specs=[pl.BlockSpec(memory_space=pl.ANY)] * 8,
        out_specs=pl.BlockSpec(memory_space=pltpu.VMEM),
        scratch_shapes=[
            pltpu.VMEM((Q, D), BF16),
            pltpu.VMEM((2 * PARENTS, D), BF16),
            pltpu.VMEM((Q, BEAM), I32),
            pltpu.VMEM((3, HID_DEV, D), BF16),
            pltpu.VMEM((1, HID_DEV), BF16),
            pltpu.VMEM((1, HID_DEV), BF16),
            pltpu.VMEM((HID, 4 * D), BF16),
            pltpu.VMEM((SERVED, Q, D), BF16),
            pltpu.VMEM((SERVED, 8, 128), BF16),
            pltpu.VMEM((SERVED, 8, 128), BF16),
            pltpu.VMEM((SERVED, 8, 128), F32),
            pltpu.VMEM((GROUPS, 8, 128), F32),
            pltpu.VMEM((2 * D, PARENTS), BF16),
            pltpu.VMEM((2 * PARENTS, D), F32),
            pltpu.VMEM((BEAM, BEAM), I32),
            pltpu.VMEM((Q, BEAM), I32),
            pltpu.VMEM((Q, BEAM), F32),
            pltpu.VMEM((Q, BEAM), F32),
            pltpu.VMEM((Q, BEAM), F32),
            pltpu.VMEM((Q, BEAM), F32),
            pltpu.VMEM((HID, 128), F32),
            pltpu.VMEM((2, 6 * D, PAIR * SLOTS), BF16),
            dma((8,)), dma(()), dma((SERVED,)), dma(()), dma((SERVED,)), dma(()), dma(()), dma(()), dma(()),
        ],
        compiler_params=pltpu.CompilerParams(collective_id=0, has_side_effects=True, vmem_limit_bytes=16 << 20),
        name="beam_scores",
    )(*[pltpu.with_memory_space_constraint(x, pltpu.HBM) for x in (
        queries, node_table, beam, w_query.T, w_node.T, w_cross.T,
        bias_hidden.reshape(1, HID_DEV), w_out.reshape(1, HID_DEV),
    )])
    return scores.T


def solution(mesh):
    in_specs = (
        P("blk", None),
        P("blk", None),
        P("blk", None),
        P(None, "hid"),
        P(None, "hid"),
        P(None, "hid"),
        P("hid"),
        P("hid"),
    )
    return jax.shard_map(shards, mesh=mesh, in_specs=in_specs, out_specs=P("blk", "hid"), check_vma=False)
```

```python
import functools

import jax
import jax.numpy as jnp
from jax import lax
from jax.experimental import pallas as pl
from jax.experimental.pallas import tpu as pltpu
from jax.sharding import PartitionSpec as P

BF16, F32, I32 = jnp.bfloat16, jnp.float32, jnp.int32
RANK = jnp.int16
GROUPS = 32
SHARES = 4
SERVED = GROUPS // SHARES
Q = 96
BEAM = 128
D = 128
HID = 256
HID_DEV = HID // SHARES
PARENTS = 1024
ROWS = 3
SLOTS = ROWS * 128
COLS = BEAM // SHARES
STEP = 32
PAIR = 2
MESH = pl.DeviceIdType.MESH


def nt(a, b):
    return lax.dot_general(a, b, (((1,), (1,)), ((), ())), preferred_element_type=F32)


def nn(a, b):
    return jnp.dot(a, b, preferred_element_type=F32)


def iota(shape, dim):
    return lax.broadcasted_iota(I32, shape, dim)


def flag(cond):
    return jnp.where(cond, 1.0, 0.0).astype(BF16)


def eye(n):
    return flag(iota((n, n), 0) == iota((n, n), 1))


def wide_row(row, copies):
    return jnp.concatenate([jnp.broadcast_to(row, (16, row.shape[1])).astype(BF16)] * copies, axis=0)


def one_hot(row, height):
    row = wide_row(row, height // 16)
    match = iota((height, row.shape[1]), 0).astype(F32).astype(BF16) == row
    return jnp.where(match, jnp.ones(row.shape, BF16), jnp.zeros(row.shape, BF16))


def list_starts(owner, even, ids):
    lower = flag(iota((Q, Q), 0) > iota((Q, Q), 1))
    ones = jnp.ones((BEAM, BEAM), BF16)
    masks = [flag((owner == o) & even) for o in ids]
    before = nn(lower, jnp.concatenate(masks, axis=1))
    tall = [
        before[:, i * BEAM : (i + 1) * BEAM] - jnp.where((owner < o) & even, 1.0, 0.0) for i, o in enumerate(ids)
    ]
    total = nn(jnp.concatenate(tall, axis=0).astype(BF16), ones)
    picked = jnp.zeros((Q, BEAM), F32)
    for i, o in enumerate(ids):
        picked = jnp.where(owner == o, total[i * Q : (i + 1) * Q], picked)
    return picked.astype(I32)


def kernel(
    q_hbm, table_hbm, beam_hbm, wq_hbm, wn_hbm, wc_hbm, bias_hbm, wout_hbm, out_ref,
    q_ref, table_ref, beam_ref, w_in, bias_in, wout_in,
    w_all, qbuf, req, reqbuf, ret, retbuf, tt, t32, keys, inner, code_s, jl_s, a_s, b_s, wo_s, joined,
    in_sem, q_send, q_recv, r_send, r_recv, w_send, w_recv, s_send, s_recv,
):
    b, h = lax.axis_index("blk"), lax.axis_index("hid")
    y, xh, z = b // 8, (b // 4) % 2, b % 4
    xl, core = h // 2, h % 2
    my_place = (y // 2) * 4 + xh * 2 + z // 2
    flip = lax.rem(xh + xl + y, 2)
    own_zl = 1 - core

    def owner_of(i):
        return (i // 2) * 8 + lax.rem(flip + i // 2, 2) * 4 + lax.rem(i, 2) * 2 + own_zl

    def server_of(i):
        return lax.rem(y + i // 2, 2) * 2 + lax.rem(z, 2)

    def source_of(k):
        return ((k // 4) * 2 + lax.rem(xl + y, 2)) * 8 + ((k // 2) % 2) * 4 + (k % 2) * 2 + core

    loads = [
        pltpu.make_async_copy(src, dst, in_sem.at[n])
        for n, (src, dst) in enumerate((
            (beam_hbm, beam_ref), (wn_hbm, w_in.at[0]), (wc_hbm, w_in.at[1]), (wq_hbm, w_in.at[2]),
            (bias_hbm, bias_in), (wout_hbm, wout_in), (q_hbm, q_ref), (table_hbm, table_ref),
        ))
    ]
    for load in loads:
        load.start()

    barrier = pltpu.get_barrier_semaphore()
    served_self = z % 2 == h

    for k in range(SERVED):
        sender = lax.rem(xl + xh + (k // 2) % 2, 2) * 2 + 1 - z % 2
        pl.semaphore_signal(barrier, inc=1, device_id={"blk": source_of(k), "hid": sender}, device_id_type=MESH)

    for d in range(1, SHARES):
        pl.semaphore_signal(barrier, inc=1, device_id={"blk": b, "hid": (h + d) % SHARES}, device_id_type=MESH)

    for load in loads[:7]:
        load.wait()

    beam = beam_ref[...]
    even = (beam & 1) == 0
    owner = beam >> 11
    local = (beam >> 1) & (PARENTS - 1)
    tall = jnp.concatenate([beam, jnp.zeros((BEAM - Q, BEAM), I32)], axis=0).T
    parent = (tall >> 1).astype(RANK)
    keys[...] = jnp.where((tall & 1) == 0, tall >> 1, 32767)

    def count(step, acc):
        for u in range(16):
            row = jnp.broadcast_to(keys[pl.ds(16 * step + u, 1), :], (16, 128)).astype(RANK)
            row = jnp.concatenate([row] * 8, axis=0)
            acc = acc + jnp.where(row < parent, jnp.ones(acc.shape, RANK), jnp.zeros(acc.shape, RANK))
        return acc

    below = lax.fori_loop(0, BEAM // 16, count, jnp.zeros((BEAM, BEAM), RANK), unroll=False)
    below = below.astype(I32).T[:Q]
    inner[...] = below

    asked = (((owner >> 2) + (owner >> 3)) & 1 == flip) & ((owner & 1) == own_zl)
    group = jnp.where(asked, (owner >> 3) * 2 + ((owner >> 1) & 1), 64)
    rank = below + list_starts(owner, even, [owner_of(i) for i in range(SERVED)])
    code_s[...] = jnp.where(even & asked, group * 4 + (rank >> 7), 64).astype(F32)
    jl_s[...] = (rank & 127).astype(F32)
    a_s[...] = (local & 255).astype(F32)
    b_s[...] = (iota((Q, BEAM), 0) + 96 * (local >> 8) - 192).astype(F32)

    ident = eye(HID_DEV)
    vectors = jnp.concatenate(
        [jnp.broadcast_to(v[...].astype(F32), (64, HID_DEV)) for v in (bias_in, wout_in)], axis=0
    ).astype(BF16)
    my_rows = pl.ds(pl.multiple_of(h * HID_DEV, HID_DEV), HID_DEV)
    for n in range(3):
        w_all[my_rows, n * D : (n + 1) * D] = w_in[n]
    w_all[my_rows, 3 * D :] = nt(ident, vectors).astype(BF16)

    row64 = iota((64, BEAM), 0)
    target = ((row64 >> 3) * 4 + (row64 & 3)).astype(F32).astype(BF16)
    is_b = ((iota((16, BEAM), 0) >> 2) & 1).astype(F32).astype(BF16)
    is_a = 1 - is_b

    def compact(step, acc):
        values, places = [], []
        for u in range(STEP):
            at = pl.ds(STEP * step + u, 1)
            payload = is_a * wide_row(a_s[at, :], 1) + is_b * wide_row(b_s[at, :], 1)
            payload = jnp.concatenate([payload] * 4, axis=0)
            values.append(jnp.where(wide_row(code_s[at, :], 4) == target, payload, 0.0).astype(BF16))
            places.append(one_hot(jl_s[at, :], BEAM))
        return acc + nt(jnp.concatenate(values, axis=1), jnp.concatenate(places, axis=1))

    tables = lax.fori_loop(0, Q // STEP, compact, jnp.zeros((64, BEAM), F32), unroll=False)
    for i in range(SERVED):
        req[i] = tables[8 * i : 8 * i + 8].astype(BF16)

    pl.semaphore_wait(barrier, SERVED + SHARES - 1)

    def all_of(ref, send_sem, recv_sem):
        return pltpu.make_async_remote_copy(
            src_ref=ref, dst_ref=ref, send_sem=send_sem, recv_sem=recv_sem,
            device_id={"blk": b, "hid": (h + 1) % SHARES}, device_id_type=MESH,
        )

    def q_copy(i):
        return pltpu.make_async_remote_copy(
            src_ref=q_ref, dst_ref=qbuf.at[my_place], send_sem=q_send, recv_sem=q_recv.at[my_place],
            device_id={"blk": owner_of(i), "hid": server_of(i)}, device_id_type=MESH,
        )

    def r_copy(i):
        return pltpu.make_async_remote_copy(
            src_ref=req.at[i], dst_ref=reqbuf.at[my_place], send_sem=r_send, recv_sem=r_recv.at[my_place],
            device_id={"blk": owner_of(i), "hid": server_of(i)}, device_id_type=MESH,
        )

    def w_copy(d):
        return pltpu.make_async_remote_copy(
            src_ref=w_all.at[my_rows], dst_ref=w_all.at[my_rows], send_sem=w_send, recv_sem=w_recv,
            device_id={"blk": b, "hid": (h + d) % SHARES}, device_id_type=MESH,
        )

    for d in range(1, SHARES):
        w_copy(d).start()

    def far(n):
        return lax.rem(y + 2 + n // 2, 4) * 2 + lax.rem(z // 2 + 1 + n, 2)

    @pl.loop(0, SERVED)
    def _(n):
        r_copy(far(n)).start()
        q_copy(far(n)).start()

    loads[7].wait()
    t32[...] = table_ref[...].astype(F32)
    ident = eye(D)
    for child in range(2):
        half = t32[pl.ds(child, PARENTS, stride=2), :].astype(BF16)
        tt[child * D : (child + 1) * D, :] = nt(ident, half).astype(BF16)

    one_row = flag(iota((D, PAIR * SLOTS), 0) == 0)
    for slot in range(2):
        joined[slot, 5 * D :] = one_row

    def s_copy(k, d):
        return pltpu.make_async_remote_copy(
            src_ref=ret.at[k], dst_ref=retbuf.at[b], send_sem=s_send, recv_sem=s_recv,
            device_id={"blk": source_of(k), "hid": d}, device_id_type=MESH,
        )

    def gather(places, slot):
        asking, wanted = [], []
        for u, k in enumerate(places):
            digits = reqbuf[k].astype(F32)
            low, rest = digits[0:4], digits[4:8] + 192.0
            high = sum(jnp.where(rest >= 96.0 * n, 1.0, 0.0) for n in (1, 2, 3))
            rest = rest + (Q * u - 96.0 * high)
            low = low + 256.0 * high
            asking += [rest[r : r + 1] for r in range(ROWS)]
            wanted += [low[r : r + 1] for r in range(ROWS)]
        asking, wanted = jnp.concatenate(asking, axis=1), jnp.concatenate(wanted, axis=1)
        hot = jnp.concatenate([one_hot(wanted - 256.0 * c, 256) for c in range(PARENTS // 256)], axis=0)
        found = nn(tt[...], hot)
        queries = nt(eye(D), jnp.concatenate([qbuf[k] for k in places], axis=0)).astype(BF16)
        query = nn(queries, one_hot(asking, Q * len(places)))
        for child in range(2):
            node = found[child * D : (child + 1) * D]
            joined[slot, 2 * child * D : (2 * child + 1) * D] = node.astype(BF16)
            joined[slot, (2 * child + 1) * D : (2 * child + 2) * D] = (node * query).astype(BF16)
        joined[slot, 4 * D : 5 * D] = query.astype(BF16)

    def score(slot):
        width = joined.shape[2] // 128
        weight = jnp.concatenate([wo_s[...]] * width, axis=1)
        shared = nn(w_all[:, 2 * D :], joined[slot, 4 * D : 6 * D])
        totals = []
        for child in range(2):
            hidden = jnp.maximum(nn(w_all[:, : 2 * D], joined[slot, 2 * child * D : 2 * (child + 1) * D]) + shared, 0.0)
            totals.append(jnp.sum(hidden * weight, axis=0, keepdims=True))
        scores = []
        for u in range(width // ROWS):
            rows = []
            for total in totals:
                rows += [total[:, r * 128 : (r + 1) * 128] for r in range(u * ROWS, (u + 1) * ROWS)]
                rows += [jnp.zeros((1, 128), F32)]
            scores.append(jnp.concatenate(rows, axis=0))
        return scores

    def near(n):
        a = lax.rem(y // 2 + n // 4, 2)
        e = lax.rem(xh + n, 2)
        return a * 4 + e * 2 + lax.rem(z // 2 + n // 2, 2)

    def arrive(places):
        for k in places:
            pltpu.make_async_remote_copy(
                src_ref=q_ref, dst_ref=qbuf.at[k], send_sem=q_send, recv_sem=q_recv.at[k],
                device_id={"blk": source_of(k), "hid": (h + 1) % SHARES}, device_id_type=MESH,
            ).wait_recv()
            pltpu.make_async_remote_copy(
                src_ref=req.at[k], dst_ref=reqbuf.at[k], send_sem=r_send, recv_sem=r_recv.at[k],
                device_id={"blk": source_of(k), "hid": (h + 1) % SHARES}, device_id_type=MESH,
            ).wait_recv()

    steps = [[near(PAIR * pair + u) for u in range(PAIR)] for pair in range(SERVED // PAIR)]
    arrive(steps[0])
    gather(steps[0], 0)
    all_of(w_all.at[: HID - HID_DEV], w_send, w_recv).wait_recv()
    wo_s[...] = jnp.broadcast_to(w_all[:, 3 * D + 64 : 3 * D + 65].astype(F32), (HID, 128))
    for pair, places in enumerate(steps):
        if pair + 1 < len(steps):
            arrive(steps[pair + 1])
        for k, scores in zip(places, score(pair % 2)):
            ret[k] = scores.astype(BF16)
        if pair + 1 < len(steps):
            gather(steps[pair + 1], (pair + 1) % 2)
        for k in places:
            for d in range(SHARES):
                here = (d == h) & (source_of(k) == b)

                @pl.when(here)
                def _():
                    retbuf[b] = ret[k]

                @pl.when(jnp.logical_not(here))
                def _():
                    s_copy(k, d).start()

    def all_owners(g, acc):
        return acc + list_starts(owner, even, [g * SERVED + i for i in range(SERVED)])

    rank = lax.fori_loop(0, GROUPS // SERVED, all_owners, inner[...], unroll=False)
    code = owner * 4 + (rank >> 7)
    mine = flag(iota((COLS, BEAM), 1) == iota((COLS, BEAM), 0) + h * COLS)
    pad = jnp.zeros((BEAM - Q, BEAM), F32)

    def columns(values):
        return nt(mine, jnp.concatenate([values.astype(F32), pad], axis=0).astype(BF16))

    code_t, jl_t = columns(code), columns((beam & 1) * 128 + (rank & 127))

    all_of(qbuf, q_send, q_recv.at[0]).wait_send()
    all_of(reqbuf, r_send, r_recv.at[0]).wait_send()
    all_of(w_all.at[: HID - HID_DEV], w_send, w_recv).wait_send()

    @pl.when(served_self)
    def _():
        all_of(retbuf.at[: GROUPS - 1], s_send, s_recv).wait_send()

    @pl.when(jnp.logical_not(served_self))
    def _():
        all_of(retbuf, s_send, s_recv).wait_send()

    @pl.when(served_self)
    def _():
        all_of(retbuf.at[: GROUPS - 1], s_send, s_recv).wait_recv()

    @pl.when(jnp.logical_not(served_self))
    def _():
        all_of(retbuf, s_send, s_recv).wait_recv()

    table = retbuf[...].astype(F32)
    table = jnp.concatenate(
        [table[:, 4 * child : 4 * child + 4, :].reshape(GROUPS * 4, 128) for child in range(2)], axis=1
    ).astype(BF16)
    slot_row = iota((GROUPS * 4, 2 * 128), 0).astype(F32)
    for c in range(0, COLS, 2):
        hot = one_hot(jnp.concatenate([jl_t[c : c + 1], jl_t[c + 1 : c + 2]], axis=1), 256)
        which = jnp.concatenate([code_t[c : c + 1], code_t[c + 1 : c + 2]], axis=1)
        seen = nn(table, hot)
        total = jnp.sum(jnp.where(slot_row == which, seen, 0.0), axis=0, keepdims=True)
        out_ref[c : c + 1, :] = total[:, :Q]
        out_ref[c + 1 : c + 2, :] = total[:, 128 : 128 + Q]


def shards(queries, node_table, beam, w_query, w_node, w_cross, bias_hidden, w_out):
    dma = pltpu.SemaphoreType.DMA
    scores = pl.pallas_call(
        kernel,
        out_shape=jax.ShapeDtypeStruct((COLS, Q), F32),
        in_specs=[pl.BlockSpec(memory_space=pl.ANY)] * 8,
        out_specs=pl.BlockSpec(memory_space=pltpu.VMEM),
        scratch_shapes=[
            pltpu.VMEM((Q, D), BF16),
            pltpu.VMEM((2 * PARENTS, D), BF16),
            pltpu.VMEM((Q, BEAM), I32),
            pltpu.VMEM((3, HID_DEV, D), BF16),
            pltpu.VMEM((1, HID_DEV), BF16),
            pltpu.VMEM((1, HID_DEV), BF16),
            pltpu.VMEM((HID, 4 * D), BF16),
            pltpu.VMEM((SERVED, Q, D), BF16),
            pltpu.VMEM((SERVED, 8, 128), BF16),
            pltpu.VMEM((SERVED, 8, 128), BF16),
            pltpu.VMEM((SERVED, 8, 128), BF16),
            pltpu.VMEM((GROUPS, 8, 128), BF16),
            pltpu.VMEM((2 * D, PARENTS), BF16),
            pltpu.VMEM((2 * PARENTS, D), F32),
            pltpu.VMEM((BEAM, BEAM), I32),
            pltpu.VMEM((Q, BEAM), I32),
            pltpu.VMEM((Q, BEAM), F32),
            pltpu.VMEM((Q, BEAM), F32),
            pltpu.VMEM((Q, BEAM), F32),
            pltpu.VMEM((Q, BEAM), F32),
            pltpu.VMEM((HID, 128), F32),
            pltpu.VMEM((2, 6 * D, PAIR * SLOTS), BF16),
            dma((8,)), dma(()), dma((SERVED,)), dma(()), dma((SERVED,)), dma(()), dma(()), dma(()), dma(()),
        ],
        compiler_params=pltpu.CompilerParams(collective_id=0, has_side_effects=True, vmem_limit_bytes=16 << 20),
        name="beam_scores",
    )(*[pltpu.with_memory_space_constraint(x, pltpu.HBM) for x in (
        queries, node_table, beam, w_query.T, w_node.T, w_cross.T,
        bias_hidden.reshape(1, HID_DEV), w_out.reshape(1, HID_DEV),
    )])
    return scores.T


def solution(mesh):
    in_specs = (
        P("blk", None),
        P("blk", None),
        P("blk", None),
        P(None, "hid"),
        P(None, "hid"),
        P(None, "hid"),
        P("hid"),
        P("hid"),
    )
    return jax.shard_map(shards, mesh=mesh, in_specs=in_specs, out_specs=P("blk", "hid"), check_vma=False)
```

```python
import functools

import jax
import jax.numpy as jnp
from jax import lax
from jax.experimental import pallas as pl
from jax.experimental.pallas import tpu as pltpu
from jax.sharding import PartitionSpec as P

BF16, F32, I32 = jnp.bfloat16, jnp.float32, jnp.int32
RANK = jnp.int16
GROUPS = 32
SHARES = 4
SERVED = GROUPS // SHARES
Q = 96
BEAM = 128
D = 128
HID = 256
HID_DEV = HID // SHARES
PARENTS = 1024
ROWS = 3
SLOTS = ROWS * 128
COLS = BEAM // SHARES
STEP = 32
PAIR = 2
MESH = pl.DeviceIdType.MESH


def nt(a, b):
    return lax.dot_general(a, b, (((1,), (1,)), ((), ())), preferred_element_type=F32)


def nn(a, b):
    return jnp.dot(a, b, preferred_element_type=F32)


def iota(shape, dim):
    return lax.broadcasted_iota(I32, shape, dim)


def flag(cond):
    return jnp.where(cond, 1.0, 0.0).astype(BF16)


def eye(n):
    return flag(iota((n, n), 0) == iota((n, n), 1))


def wide_row(row, copies):
    return jnp.concatenate([jnp.broadcast_to(row, (16, row.shape[1])).astype(BF16)] * copies, axis=0)


def one_hot(row, height):
    row = wide_row(row, height // 16)
    match = iota((height, row.shape[1]), 0).astype(F32).astype(BF16) == row
    return jnp.where(match, jnp.ones(row.shape, BF16), jnp.zeros(row.shape, BF16))


def list_starts(owner, even, ids):
    lower = flag(iota((Q, Q), 0) > iota((Q, Q), 1))
    ones = jnp.ones((BEAM, BEAM), BF16)
    masks = [flag((owner == o) & even) for o in ids]
    before = nn(lower, jnp.concatenate(masks, axis=1))
    tall = [
        before[:, i * BEAM : (i + 1) * BEAM] - jnp.where((owner < o) & even, 1.0, 0.0) for i, o in enumerate(ids)
    ]
    total = nn(jnp.concatenate(tall, axis=0).astype(BF16), ones)
    picked = jnp.zeros((Q, BEAM), F32)
    for i, o in enumerate(ids):
        picked = jnp.where(owner == o, total[i * Q : (i + 1) * Q], picked)
    return picked.astype(I32)


def kernel(
    q_hbm, table_hbm, beam_hbm, wq_hbm, wn_hbm, wc_hbm, bias_hbm, wout_hbm, out_ref,
    q_ref, table_ref, beam_ref, w_in, bias_in, wout_in,
    w_all, qbuf, req, reqbuf, ret, retbuf, tt, t32, keys, inner, code_s, jl_s, a_s, b_s, wo_s, joined,
    in_sem, q_send, q_recv, r_send, r_recv, w_send, w_recv, s_send, s_recv,
):
    b, h = lax.axis_index("blk"), lax.axis_index("hid")
    y, xh, z = b // 8, (b // 4) % 2, b % 4
    xl, core = h // 2, h % 2
    my_place = (y // 2) * 4 + xh * 2 + z // 2
    flip = lax.rem(xh + xl + y, 2)
    own_zl = 1 - core

    def owner_of(i):
        return (i // 2) * 8 + lax.rem(flip + i // 2, 2) * 4 + lax.rem(i, 2) * 2 + own_zl

    def server_of(i):
        return lax.rem(y + i // 2, 2) * 2 + lax.rem(z, 2)

    def source_of(k):
        return ((k // 4) * 2 + lax.rem(xl + y, 2)) * 8 + ((k // 2) % 2) * 4 + (k % 2) * 2 + core

    loads = [
        pltpu.make_async_copy(src, dst, in_sem.at[n])
        for n, (src, dst) in enumerate((
            (beam_hbm, beam_ref), (wn_hbm, w_in.at[0]), (wc_hbm, w_in.at[1]), (wq_hbm, w_in.at[2]),
            (bias_hbm, bias_in), (wout_hbm, wout_in), (q_hbm, q_ref), (table_hbm, table_ref),
        ))
    ]
    for load in loads:
        load.start()

    barrier = pltpu.get_barrier_semaphore()
    served_self = z % 2 == h

    for k in range(SERVED):
        sender = lax.rem(xl + xh + (k // 2) % 2, 2) * 2 + 1 - z % 2
        pl.semaphore_signal(barrier, inc=1, device_id={"blk": source_of(k), "hid": sender}, device_id_type=MESH)

    for d in range(1, SHARES):
        pl.semaphore_signal(barrier, inc=1, device_id={"blk": b, "hid": (h + d) % SHARES}, device_id_type=MESH)

    for load in loads[:7]:
        load.wait()

    beam = beam_ref[...]
    even = (beam & 1) == 0
    owner = beam >> 11
    local = (beam >> 1) & (PARENTS - 1)
    tall = jnp.concatenate([beam, jnp.zeros((BEAM - Q, BEAM), I32)], axis=0).T
    parent = (tall >> 1).astype(RANK)
    keys[...] = jnp.where((tall & 1) == 0, tall >> 1, 32767)

    def count(step, acc):
        for u in range(16):
            row = jnp.broadcast_to(keys[pl.ds(16 * step + u, 1), :], (16, 128)).astype(RANK)
            row = jnp.concatenate([row] * 8, axis=0)
            acc = acc + jnp.where(row < parent, jnp.ones(acc.shape, RANK), jnp.zeros(acc.shape, RANK))
        return acc

    below = lax.fori_loop(0, BEAM // 16, count, jnp.zeros((BEAM, BEAM), RANK), unroll=False)
    below = below.astype(I32).T[:Q]
    inner[...] = below

    asked = (((owner >> 2) + (owner >> 3)) & 1 == flip) & ((owner & 1) == own_zl)
    group = jnp.where(asked, (owner >> 3) * 2 + ((owner >> 1) & 1), 64)
    rank = below + list_starts(owner, even, [owner_of(i) for i in range(SERVED)])
    code_s[...] = jnp.where(even & asked, group * 4 + (rank >> 7), 64).astype(F32)
    jl_s[...] = (rank & 127).astype(F32)
    a_s[...] = (local & 255).astype(F32)
    b_s[...] = (iota((Q, BEAM), 0) + 96 * (local >> 8) - 192).astype(F32)

    ident = eye(HID_DEV)
    vectors = jnp.concatenate(
        [jnp.broadcast_to(v[...].astype(F32), (64, HID_DEV)) for v in (bias_in, wout_in)], axis=0
    ).astype(BF16)
    my_rows = pl.ds(pl.multiple_of(h * HID_DEV, HID_DEV), HID_DEV)
    for n in range(3):
        w_all[my_rows, n * D : (n + 1) * D] = w_in[n]
    w_all[my_rows, 3 * D :] = nt(ident, vectors).astype(BF16)

    row64 = iota((64, BEAM), 0)
    target = ((row64 >> 3) * 4 + (row64 & 3)).astype(F32).astype(BF16)
    is_b = ((iota((16, BEAM), 0) >> 2) & 1).astype(F32).astype(BF16)
    is_a = 1 - is_b

    def compact(step, acc):
        values, places = [], []
        for u in range(STEP):
            at = pl.ds(STEP * step + u, 1)
            payload = is_a * wide_row(a_s[at, :], 1) + is_b * wide_row(b_s[at, :], 1)
            payload = jnp.concatenate([payload] * 4, axis=0)
            values.append(jnp.where(wide_row(code_s[at, :], 4) == target, payload, 0.0).astype(BF16))
            places.append(one_hot(jl_s[at, :], BEAM))
        return acc + nt(jnp.concatenate(values, axis=1), jnp.concatenate(places, axis=1))

    tables = lax.fori_loop(0, Q // STEP, compact, jnp.zeros((64, BEAM), F32), unroll=False)
    for i in range(SERVED):
        req[i] = tables[8 * i : 8 * i + 8].astype(BF16)

    pl.semaphore_wait(barrier, SERVED + SHARES - 1)

    def all_of(ref, send_sem, recv_sem):
        return pltpu.make_async_remote_copy(
            src_ref=ref, dst_ref=ref, send_sem=send_sem, recv_sem=recv_sem,
            device_id={"blk": b, "hid": (h + 1) % SHARES}, device_id_type=MESH,
        )

    def q_copy(i):
        return pltpu.make_async_remote_copy(
            src_ref=q_ref, dst_ref=qbuf.at[my_place], send_sem=q_send, recv_sem=q_recv.at[my_place],
            device_id={"blk": owner_of(i), "hid": server_of(i)}, device_id_type=MESH,
        )

    def r_copy(i):
        return pltpu.make_async_remote_copy(
            src_ref=req.at[i], dst_ref=reqbuf.at[my_place], send_sem=r_send, recv_sem=r_recv.at[my_place],
            device_id={"blk": owner_of(i), "hid": server_of(i)}, device_id_type=MESH,
        )

    def w_copy(d):
        return pltpu.make_async_remote_copy(
            src_ref=w_all.at[my_rows], dst_ref=w_all.at[my_rows], send_sem=w_send, recv_sem=w_recv,
            device_id={"blk": b, "hid": (h + d) % SHARES}, device_id_type=MESH,
        )

    for d in range(1, SHARES):
        w_copy(d).start()

    def ahead(n):
        return lax.rem(y + n // 2, 4) * 2 + lax.rem(z // 2 + n, 2)

    @pl.loop(0, SERVED)
    def _(n):
        r_copy(ahead(n)).start()
        q_copy(ahead(n)).start()

    loads[7].wait()
    t32[...] = table_ref[...].astype(F32)
    ident = eye(D)
    for child in range(2):
        half = t32[pl.ds(child, PARENTS, stride=2), :].astype(BF16)
        tt[child * D : (child + 1) * D, :] = nt(ident, half).astype(BF16)

    one_row = flag(iota((D, PAIR * SLOTS), 0) == 0)
    for slot in range(2):
        joined[slot, 5 * D :] = one_row

    def s_copy(k, d):
        return pltpu.make_async_remote_copy(
            src_ref=ret.at[k], dst_ref=retbuf.at[b], send_sem=s_send, recv_sem=s_recv,
            device_id={"blk": source_of(k), "hid": d}, device_id_type=MESH,
        )

    def gather(places, slot):
        asking, wanted = [], []
        for u, k in enumerate(places):
            digits = reqbuf[k].astype(F32)
            low, rest = digits[0:4], digits[4:8] + 192.0
            high = sum(jnp.where(rest >= 96.0 * n, 1.0, 0.0) for n in (1, 2, 3))
            rest = rest + (Q * u - 96.0 * high)
            low = low + 256.0 * high
            asking += [rest[r : r + 1] for r in range(ROWS)]
            wanted += [low[r : r + 1] for r in range(ROWS)]
        asking, wanted = jnp.concatenate(asking, axis=1), jnp.concatenate(wanted, axis=1)
        hot = jnp.concatenate([one_hot(wanted - 256.0 * c, 256) for c in range(PARENTS // 256)], axis=0)
        found = nn(tt[...], hot)
        queries = nt(eye(D), jnp.concatenate([qbuf[k] for k in places], axis=0)).astype(BF16)
        query = nn(queries, one_hot(asking, Q * len(places)))
        for child in range(2):
            node = found[child * D : (child + 1) * D]
            joined[slot, 2 * child * D : (2 * child + 1) * D] = node.astype(BF16)
            joined[slot, (2 * child + 1) * D : (2 * child + 2) * D] = (node * query).astype(BF16)
        joined[slot, 4 * D : 5 * D] = query.astype(BF16)

    def score(slot):
        width = joined.shape[2] // 128
        weight = jnp.concatenate([wo_s[...]] * width, axis=1)
        shared = nn(w_all[:, 2 * D :], joined[slot, 4 * D : 6 * D])
        totals = []
        for child in range(2):
            hidden = jnp.maximum(nn(w_all[:, : 2 * D], joined[slot, 2 * child * D : 2 * (child + 1) * D]) + shared, 0.0)
            totals.append(jnp.sum(hidden * weight, axis=0, keepdims=True))
        scores = []
        for u in range(width // ROWS):
            rows = []
            for total in totals:
                rows += [total[:, r * 128 : (r + 1) * 128] for r in range(u * ROWS, (u + 1) * ROWS)]
                rows += [jnp.zeros((1, 128), F32)]
            scores.append(jnp.concatenate(rows, axis=0))
        return scores

    def near(n):
        a = lax.rem(y // 2 + n // 4, 2)
        e = lax.rem(xh + n, 2)
        return a * 4 + e * 2 + lax.rem(z // 2 + n // 2, 2)

    def arrive(places):
        for k in places:
            pltpu.make_async_remote_copy(
                src_ref=q_ref, dst_ref=qbuf.at[k], send_sem=q_send, recv_sem=q_recv.at[k],
                device_id={"blk": source_of(k), "hid": (h + 1) % SHARES}, device_id_type=MESH,
            ).wait_recv()
            pltpu.make_async_remote_copy(
                src_ref=req.at[k], dst_ref=reqbuf.at[k], send_sem=r_send, recv_sem=r_recv.at[k],
                device_id={"blk": source_of(k), "hid": (h + 1) % SHARES}, device_id_type=MESH,
            ).wait_recv()

    steps = [[near(PAIR * pair + u) for u in range(PAIR)] for pair in range(SERVED // PAIR)]
    arrive(steps[0])
    gather(steps[0], 0)
    all_of(w_all.at[: HID - HID_DEV], w_send, w_recv).wait_recv()
    wo_s[...] = jnp.broadcast_to(w_all[:, 3 * D + 64 : 3 * D + 65].astype(F32), (HID, 128))
    for pair, places in enumerate(steps):
        if pair + 1 < len(steps):
            arrive(steps[pair + 1])
        for k, scores in zip(places, score(pair % 2)):
            ret[k] = scores.astype(BF16)
        if pair + 1 < len(steps):
            gather(steps[pair + 1], (pair + 1) % 2)
        for k in places:
            for d in range(SHARES):
                here = (d == h) & (source_of(k) == b)

                @pl.when(here)
                def _():
                    retbuf[b] = ret[k]

                @pl.when(jnp.logical_not(here))
                def _():
                    s_copy(k, d).start()

    def all_owners(g, acc):
        return acc + list_starts(owner, even, [g * SERVED + i for i in range(SERVED)])

    rank = lax.fori_loop(0, GROUPS // SERVED, all_owners, inner[...], unroll=False)
    code = owner * 4 + (rank >> 7)
    mine = flag(iota((COLS, BEAM), 1) == iota((COLS, BEAM), 0) + h * COLS)
    pad = jnp.zeros((BEAM - Q, BEAM), F32)

    def columns(values):
        return nt(mine, jnp.concatenate([values.astype(F32), pad], axis=0).astype(BF16))

    code_t, jl_t = columns(code), columns((beam & 1) * 128 + (rank & 127))

    all_of(qbuf, q_send, q_recv.at[0]).wait_send()
    all_of(reqbuf, r_send, r_recv.at[0]).wait_send()
    all_of(w_all.at[: HID - HID_DEV], w_send, w_recv).wait_send()

    @pl.when(served_self)
    def _():
        all_of(retbuf.at[: GROUPS - 1], s_send, s_recv).wait_send()

    @pl.when(jnp.logical_not(served_self))
    def _():
        all_of(retbuf, s_send, s_recv).wait_send()

    @pl.when(served_self)
    def _():
        all_of(retbuf.at[: GROUPS - 1], s_send, s_recv).wait_recv()

    @pl.when(jnp.logical_not(served_self))
    def _():
        all_of(retbuf, s_send, s_recv).wait_recv()

    table = retbuf[...].astype(F32)
    table = jnp.concatenate(
        [table[:, 4 * child : 4 * child + 4, :].reshape(GROUPS * 4, 128) for child in range(2)], axis=1
    ).astype(BF16)
    slot_row = iota((GROUPS * 4, 2 * 128), 0).astype(F32)
    for c in range(0, COLS, 2):
        hot = one_hot(jnp.concatenate([jl_t[c : c + 1], jl_t[c + 1 : c + 2]], axis=1), 256)
        which = jnp.concatenate([code_t[c : c + 1], code_t[c + 1 : c + 2]], axis=1)
        seen = nn(table, hot)
        total = jnp.sum(jnp.where(slot_row == which, seen, 0.0), axis=0, keepdims=True)
        out_ref[c : c + 1, :] = total[:, :Q]
        out_ref[c + 1 : c + 2, :] = total[:, 128 : 128 + Q]


def shards(queries, node_table, beam, w_query, w_node, w_cross, bias_hidden, w_out):
    dma = pltpu.SemaphoreType.DMA
    scores = pl.pallas_call(
        kernel,
        out_shape=jax.ShapeDtypeStruct((COLS, Q), F32),
        in_specs=[pl.BlockSpec(memory_space=pl.ANY)] * 8,
        out_specs=pl.BlockSpec(memory_space=pltpu.VMEM),
        scratch_shapes=[
            pltpu.VMEM((Q, D), BF16),
            pltpu.VMEM((2 * PARENTS, D), BF16),
            pltpu.VMEM((Q, BEAM), I32),
            pltpu.VMEM((3, HID_DEV, D), BF16),
            pltpu.VMEM((1, HID_DEV), BF16),
            pltpu.VMEM((1, HID_DEV), BF16),
            pltpu.VMEM((HID, 4 * D), BF16),
            pltpu.VMEM((SERVED, Q, D), BF16),
            pltpu.VMEM((SERVED, 8, 128), BF16),
            pltpu.VMEM((SERVED, 8, 128), BF16),
            pltpu.VMEM((SERVED, 8, 128), BF16),
            pltpu.VMEM((GROUPS, 8, 128), BF16),
            pltpu.VMEM((2 * D, PARENTS), BF16),
            pltpu.VMEM((2 * PARENTS, D), F32),
            pltpu.VMEM((BEAM, BEAM), I32),
            pltpu.VMEM((Q, BEAM), I32),
            pltpu.VMEM((Q, BEAM), F32),
            pltpu.VMEM((Q, BEAM), F32),
            pltpu.VMEM((Q, BEAM), F32),
            pltpu.VMEM((Q, BEAM), F32),
            pltpu.VMEM((HID, 128), F32),
            pltpu.VMEM((2, 6 * D, PAIR * SLOTS), BF16),
            dma((8,)), dma(()), dma((SERVED,)), dma(()), dma((SERVED,)), dma(()), dma(()), dma(()), dma(()),
        ],
        compiler_params=pltpu.CompilerParams(collective_id=0, has_side_effects=True, vmem_limit_bytes=16 << 20),
        name="beam_scores",
    )(*[pltpu.with_memory_space_constraint(x, pltpu.HBM) for x in (
        queries, node_table, beam, w_query.T, w_node.T, w_cross.T,
        bias_hidden.reshape(1, HID_DEV), w_out.reshape(1, HID_DEV),
    )])
    return scores.T


def solution(mesh):
    in_specs = (
        P("blk", None),
        P("blk", None),
        P("blk", None),
        P(None, "hid"),
        P(None, "hid"),
        P(None, "hid"),
        P("hid"),
        P("hid"),
    )
    return jax.shard_map(shards, mesh=mesh, in_specs=in_specs, out_specs=P("blk", "hid"), check_vma=False)
```
